32 devices in a mesh: seq: 8 (over z, x), head: 4 (over y, core).
Axes of the slice: x: 2, y: 2, z: 4, core: 2. Of those that a mesh axis runs over, the one named last changes fastest.
Arguments:
- queries: bfloat16 [1024, 2048], P('seq', 'head'), may hold values from -5 to 5
- key_rows: bfloat16 [1024, 2048], P('seq', 'head'), may hold values from -5 to 5
- value_rows: bfloat16 [1024, 2048], P('seq', 'head'), may hold values from -6 to 6
- out_weight: bfloat16 [2048, 2048], P('head'), may hold values from -0.125 to 0.125
- grad_out: bfloat16 [1024, 2048], P('seq', 'head'), may hold values from -6 to 6
- pair_offsets: int32 [16], replicated, may hold values from 0 to 1
- far_head_offsets: int32 [16], replicated, may hold values from 0 to 3
Outputs:
- layer_out: bfloat16 [1024, 2048], P('seq')
- grad_queries: bfloat16 [1024, 2048], P('seq', 'head')
- grad_keys: bfloat16 [1024, 2048], P('seq', 'head')
- grad_values: bfloat16 [1024, 2048], P('seq', 'head')
The draws below stay inside these ranges and needn't reach their ends.
All inputs are finite; a program needn't handle non-finite values.
Results may differ from the reference program's by a relative error of at most 0.009.
Values may be sent and summed in bfloat16 or wider, within the bound.
No kernel may reach another device: no remote copies, remote signals or barrier semaphores. Data moves between devices by JAX's collectives and lax.ppermute only.
A program may use at most 64 MiB of HBM per device.

```python
import jax
import jax.numpy as jnp
from jax import lax

D = 2048
ATTENTION_HEADS = 16
HEAD_DIM = 128
TOKENS = 1024
SELECTED = 256
FAR_DILATION = 4
N_HEAD = 4


def drawn_draws(key):
    base_key = jax.random.fold_in(key, 7101)
    query_key, keys_key = jax.random.split(base_key, 2)
    queries = jax.random.truncated_normal(query_key, -4.5, 4.5, (TOKENS, D), jnp.float32)
    key_rows = jax.random.truncated_normal(keys_key, -4.5, 4.5, (TOKENS, D), jnp.float32)
    return (queries, key_rows)


def draw_queries(key, part):
    return drawn_draws(key)[0].astype(jnp.bfloat16)


def draw_key_rows(key, part):
    return drawn_draws(key)[1].astype(jnp.bfloat16)


def plant(values, own_key, smallest, high):
    index_at = [jax.random.randint(jax.random.fold_in(own_key, axis), (), 0, length) for axis, length in enumerate(values.shape)]
    longest = values.shape.index(max(values.shape))
    next_to = index_at[:longest] + [(index_at[longest] + 1) % values.shape[longest]] + index_at[longest + 1:]
    return values.at[tuple(index_at)].set(smallest).at[tuple(next_to)].set(high)


def level_of(own_key, dims, pieces, smallest, top_value):
    loudness = 1.0
    for dim, shards_of in pieces:
        steps = jax.random.uniform(jax.random.fold_in(jax.random.fold_in(own_key, 6), dim), (shards_of,), jnp.float32, smallest / len(pieces), top_value / len(pieces))
        loudness = loudness * jnp.repeat(jnp.exp(steps), dims[dim] // shards_of).reshape((-1,) + (1,) * (len(dims) - 1 - dim))
    return loudness


def noise(key, extent, width, limit, shards=(), dtype=jnp.bfloat16):
    values = jax.random.normal(key, extent, jnp.float32) * width
    if len(shards) > 0:
        values = level_of(key, extent, shards, -0.22, 0.18) * values
    return jnp.clip(values, min=-limit, max=limit).astype(dtype)


def setup_inputs(seed: int = 0) -> dict:
    splits = jax.random.split(jax.random.key(seed), 8)
    queries = draw_queries(jax.random.fold_in(splits[7], 71), 0)
    key_rows = draw_key_rows(jax.random.fold_in(splits[7], 71), 0)
    value_rows = noise(splits[2], (TOKENS, D), 1.0, 6.0, ((0, 8), (1, 4)))
    out_weight = noise(splits[3], (D, D), D ** -0.5, 0.125, ((0, 4),))
    grad_out = noise(splits[4], (TOKENS, D), 1.0, 6.0, ((0, 8), (1, 4)))
    pair_offsets = plant(jax.random.randint(splits[5], (ATTENTION_HEADS,), 0, 2), jax.random.fold_in(splits[5], 1), 0, 1).astype(jnp.int32)
    far_head_offsets = plant(jax.random.randint(splits[6], (ATTENTION_HEADS,), 0, FAR_DILATION), jax.random.fold_in(splits[6], 1), 0, FAR_DILATION - 1).astype(jnp.int32)
    return dict(queries=queries, key_rows=key_rows, value_rows=value_rows, out_weight=out_weight, grad_out=grad_out, pair_offsets=pair_offsets, far_head_offsets=far_head_offsets)


masked_score = -1.0e30


def to_float(tensor):
    return tensor.astype(jnp.float32)


def round_trip(tensor):
    return lax.optimization_barrier(tensor.astype(jnp.bfloat16)).astype(jnp.float32)


def select(tensor, token_stride, start_offset):
    layout = (tensor.shape[0] // (SELECTED * token_stride), SELECTED, token_stride) + tensor.shape[1:]
    return lax.dynamic_index_in_dim(tensor.reshape(layout), start_offset, axis=2, keepdims=False)


def spread(entries, token_stride, start_offset, filler):
    layout = entries.shape[:2] + (token_stride,) + entries.shape[2:]
    lane_ids = lax.broadcasted_iota(jnp.int32, layout, 2)
    placed = jnp.where(lane_ids == start_offset, jnp.expand_dims(entries, 2), filler)
    return placed.reshape((layout[0] * layout[1] * token_stride,) + entries.shape[2:])


def causal_scores(query_part, key_part):
    number = query_part.shape[1]
    scores = jnp.einsum("sid,sjd->sij", to_float(query_part), to_float(key_part)) * (HEAD_DIM ** -0.5)
    row_ids = lax.broadcasted_iota(jnp.int32, (number, number), 0)
    col_ids = lax.broadcasted_iota(jnp.int32, (number, number), 1)
    return jnp.where(row_ids >= col_ids, scores, masked_score)


def head_forward(operands):
    head_query, head_key, head_value, pair_branch_shift, far_branch_shift = operands
    branches = []
    for token_stride, start_offset in ((1, 0), (2, pair_branch_shift), (FAR_DILATION, far_branch_shift)):
        scores = causal_scores(select(head_query, token_stride, start_offset), select(head_key, token_stride, start_offset))
        branch_max = jnp.max(scores, axis=-1)
        weights = jnp.exp(scores - branch_max[..., None])
        branch_sum = jnp.sum(weights, axis=-1)
        numerator = jnp.einsum("sij,sjd->sid", round_trip(weights), to_float(select(head_value, token_stride, start_offset)))
        branches.append((spread(branch_max, token_stride, start_offset, masked_score), spread(branch_sum, token_stride, start_offset, 0.0), spread(numerator, token_stride, start_offset, 0.0)))
    row_max = jnp.maximum(jnp.maximum(branches[0][0], branches[1][0]), branches[2][0])
    row_sum = jnp.zeros_like(row_max)
    numerator = jnp.zeros_like(branches[0][2])
    for branch in branches:
        rescale = jnp.exp(branch[0] - row_max)
        row_sum = row_sum + branch[1] * rescale
        numerator = numerator + branch[2] * rescale[:, None]
    return numerator / row_sum[:, None], row_max, row_sum


def head_backward(operands):
    head_query, head_key, head_value, head_grad, head_out, row_max, row_sum, pair_branch_shift, far_branch_shift = operands
    factor = HEAD_DIM ** -0.5
    row_delta = jnp.sum(to_float(head_grad) * head_out, axis=-1)
    query_grad = jnp.zeros_like(head_out)
    key_grad = jnp.zeros_like(head_out)
    value_grad = jnp.zeros_like(head_out)
    for token_stride, start_offset in ((1, 0), (2, pair_branch_shift), (FAR_DILATION, far_branch_shift)):
        query_part = select(head_query, token_stride, start_offset)
        key_part = select(head_key, token_stride, start_offset)
        value_part = select(head_value, token_stride, start_offset)
        grad_part = select(head_grad, token_stride, start_offset)
        scores = causal_scores(query_part, key_part)
        probability = jnp.exp(scores - select(row_max, token_stride, start_offset)[..., None]) / select(row_sum, token_stride, start_offset)[..., None]
        branch_dv = jnp.einsum("sij,sid->sjd", round_trip(probability), to_float(grad_part))
        prob_grad = jnp.einsum("sid,sjd->sij", to_float(grad_part), to_float(value_part))
        score_grad = round_trip(probability * (prob_grad - select(row_delta, token_stride, start_offset)[..., None]))
        branch_dq = jnp.einsum("sij,sjd->sid", score_grad, to_float(key_part)) * factor
        branch_dk = jnp.einsum("sij,sid->sjd", score_grad, to_float(query_part)) * factor
        query_grad = query_grad + spread(branch_dq, token_stride, start_offset, 0.0)
        key_grad = key_grad + spread(branch_dk, token_stride, start_offset, 0.0)
        value_grad = value_grad + spread(branch_dv, token_stride, start_offset, 0.0)
    return query_grad, key_grad, value_grad


def by_head(tensor):
    return tensor.reshape(TOKENS, ATTENTION_HEADS, HEAD_DIM).transpose(1, 0, 2)


def by_token(tensor):
    return tensor.transpose(1, 0, 2).reshape(TOKENS, ATTENTION_HEADS * HEAD_DIM)


def reference(queries, key_rows, value_rows, out_weight, grad_out, pair_offsets, far_head_offsets):
    head_queries = by_head(queries)
    head_keys = by_head(key_rows)
    head_values = by_head(value_rows)
    head_out, row_max, row_sum = lax.map(head_forward, (head_queries, head_keys, head_values, pair_offsets, far_head_offsets))
    attended = by_token(head_out).astype(jnp.bfloat16)
    slab_width = D // N_HEAD
    layer_sum = jnp.zeros((TOKENS, D), jnp.float32)
    for part_index in range(N_HEAD):
        lower = part_index * slab_width
        partial_out = jnp.dot(attended[:, lower:lower + slab_width], out_weight[lower:lower + slab_width], preferred_element_type=jnp.float32)
        layer_sum = layer_sum + round_trip(partial_out)
    layer_out = layer_sum.astype(jnp.bfloat16)
    grad_attended = jnp.dot(grad_out, out_weight.T, preferred_element_type=jnp.float32).astype(jnp.bfloat16)
    query_grad, key_grad, value_grad = lax.map(head_backward, (head_queries, head_keys, head_values, by_head(grad_attended), head_out, row_max, row_sum, pair_offsets, far_head_offsets))
    return (layer_out, by_token(query_grad).astype(jnp.bfloat16), by_token(key_grad).astype(jnp.bfloat16), by_token(value_grad).astype(jnp.bfloat16))
```

```python
import jax
import jax.numpy as jnp
from jax import lax
from jax.experimental import pallas as pl
from jax.experimental.pallas import tpu as pltpu
from jax.sharding import PartitionSpec as P

HEAD_DIM = 128
SPAN = 512


masked_score = -1e30


def shortened(array):
    return jax.tree.map(lambda a: a.astype(jnp.bfloat16) if a.dtype == jnp.float32 else a, array)


def partner(value, axis, distance):
    mask = 2**distance
    pairs = [(source, source ^ mask) for source in range(lax.axis_size(axis))]
    return lax.ppermute(value, axis, pairs)


def select(tensor, token_stride, start_offset):
    head_count = tensor.shape[0]
    number = tensor.shape[1] // token_stride
    shaped = tensor.reshape((head_count, number, token_stride) + tensor.shape[2:])
    lane_ids = lax.broadcasted_iota(jnp.int32, shaped.shape, 2)
    chosen = start_offset.reshape((head_count, 1, 1) + (1,) * (tensor.ndim - 2))
    return jnp.sum(jnp.where(lane_ids == chosen, shaped, jnp.zeros((), tensor.dtype)), axis=2)


def spread(entries, token_stride, start_offset, filler):
    head_count = entries.shape[0]
    number = entries.shape[1]
    layout = (head_count, number, token_stride) + entries.shape[2:]
    lane_ids = lax.broadcasted_iota(jnp.int32, layout, 2)
    chosen = start_offset.reshape((head_count, 1, 1) + (1,) * (entries.ndim - 2))
    placed = jnp.where(lane_ids == chosen, jnp.expand_dims(entries, 2), filler)
    return placed.reshape((head_count, number * token_stride) + entries.shape[2:])


def product(left_side, right_side, pattern):
    return jnp.einsum(pattern, left_side, right_side, preferred_element_type=jnp.float32)


def masked(query_part, key_part, first_row, first_col, factor):
    scores = product(query_part, key_part, "hid,hjd->hij") * factor
    row_ids = first_row + lax.broadcasted_iota(jnp.int32, scores.shape, 1)
    col_ids = first_col + lax.broadcasted_iota(jnp.int32, scores.shape, 2)
    return jnp.where(row_ids >= col_ids, scores, masked_score)


def branch_stats(scores, value_part):
    branch_max = jnp.max(scores, axis=-1)
    weights = jnp.exp(scores - branch_max[..., None])
    numerator = product(weights.astype(jnp.bfloat16), value_part, "hij,hjd->hid")
    return (branch_max, jnp.sum(weights, axis=-1), numerator)


def score_grads(scores, row_max, row_sum, grad_part, value_part, row_delta):
    probability = jnp.exp(scores - row_max[..., None]) / row_sum[..., None]
    prob_grad = product(grad_part, value_part, "hid,hjd->hij")
    score_grad = (probability * (prob_grad - row_delta[..., None])).astype(jnp.bfloat16)
    return (probability.astype(jnp.bfloat16), score_grad)


def exchange_local(queries, key_rows, value_rows, out_weight, grad_out, pair_offsets, far_head_offsets):
    tokens = queries.shape[0]
    head_count = queries.shape[1] // HEAD_DIM
    factor = HEAD_DIM ** (-0.5)
    seq_count = lax.axis_size("seq")
    total = tokens * seq_count
    selected = min(SPAN, total // 4)
    local_group = selected // tokens
    local_levels = local_group.bit_length() - 1
    dilation = total // selected
    far_rows = tokens // dilation
    half_rows = tokens // 2
    position = lax.axis_index("seq")
    local_rank = position % local_group
    pair_rank = position % (2 * local_group)
    head_group = lax.axis_index("head")
    pair_branch_shift = lax.dynamic_slice_in_dim(pair_offsets, head_group * head_count, head_count)
    far_branch_shift = lax.dynamic_slice_in_dim(
        far_head_offsets, head_group * head_count, head_count
    )

    def by_head(tensor):
        return tensor.reshape(tokens, head_count, HEAD_DIM).transpose(1, 0, 2)

    def by_token(tensor):
        return tensor.transpose(1, 0, 2).reshape(tokens, head_count * HEAD_DIM)

    def stacked(mine, theirs, bit):
        high = position // 2**bit % 2 == 1
        lower = jnp.where(high, theirs, mine)
        upper = jnp.where(high, mine, theirs)
        return jnp.concatenate([lower, upper], axis=1)

    def joined(mine, theirs, bit):
        return tuple((stacked(first, second, bit) for first, second in zip(mine, theirs)))

    head_queries = by_head(queries)
    head_keys = by_head(key_rows)
    head_values = by_head(value_rows)
    parts = (head_keys, head_values)
    for bit in range(local_levels):
        parts = joined(
            parts,
            jax.tree.map(
                lambda part, own: part.astype(own.dtype),
                partner(shortened(parts), "seq", bit),
                parts,
            ),
            bit,
        )
    segment_key, segment_value = parts
    local_scores = masked(head_queries, segment_key, local_rank * tokens, 0, factor)
    local_stats = branch_stats(local_scores, segment_value)
    pair_query = select(head_queries, 2, pair_branch_shift)
    pair_key = select(head_keys, 2, pair_branch_shift)
    pair_value = select(head_values, 2, pair_branch_shift)
    nearby = (
        select(segment_key, 2, pair_branch_shift),
        select(segment_value, 2, pair_branch_shift),
    )
    pair_all_key, pair_all_value = joined(
        nearby, partner((nearby[0], nearby[1]), "seq", local_levels), local_levels
    )
    pair_scores = masked(pair_query, pair_all_key, pair_rank * half_rows, 0, factor)
    pair_stats = branch_stats(pair_scores, pair_all_value)
    far_query = select(head_queries, dilation, far_branch_shift)
    far_key = select(head_keys, dilation, far_branch_shift)
    far_value = select(head_values, dilation, far_branch_shift)
    every_key, every_value = (
        lax.all_gather(far_key, "seq", axis=1, tiled=True),
        lax.all_gather(far_value, "seq", axis=1, tiled=True),
    )
    far_scores = masked(far_query, every_key, position * far_rows, 0, factor)
    far_stats = branch_stats(far_scores, every_value)
    pair_spread = (
        spread(pair_stats[0], 2, pair_branch_shift, masked_score),
        spread(pair_stats[1], 2, pair_branch_shift, 0.0),
        spread(pair_stats[2], 2, pair_branch_shift, 0.0),
    )
    far_spread = (
        spread(far_stats[0], dilation, far_branch_shift, masked_score),
        spread(far_stats[1], dilation, far_branch_shift, 0.0),
        spread(far_stats[2], dilation, far_branch_shift, 0.0),
    )
    row_max = jnp.maximum(jnp.maximum(local_stats[0], pair_spread[0]), far_spread[0])
    row_sum = jnp.zeros_like(row_max)
    numerator = jnp.zeros_like(local_stats[2])
    for branch in (local_stats, pair_spread, far_spread):
        rescale = jnp.exp(branch[0] - row_max)
        row_sum = row_sum + branch[1] * rescale
        numerator = numerator + branch[2] * rescale[..., None]
    head_out = numerator / row_sum[..., None]
    attended = by_token(head_out).astype(jnp.bfloat16)
    partial_out = jnp.dot(attended, out_weight, preferred_element_type=jnp.float32)
    layer_out = lax.psum(partial_out.astype(jnp.bfloat16), "head")
    grad_attended = lax.dot_general(
        lax.all_gather(grad_out, "head", axis=1, tiled=True),
        out_weight,
        (((1,), (1,)), ((), ())),
        preferred_element_type=jnp.float32,
    )
    head_grads = by_head(grad_attended.astype(jnp.bfloat16))
    row_delta = jnp.sum(head_grads.astype(jnp.float32) * head_out, axis=-1)
    _, local_dscore = score_grads(
        local_scores, row_max, row_sum, head_grads, segment_value, row_delta
    )
    query_grad = product(local_dscore, segment_key, "hij,hjd->hid") * factor
    parts = (head_queries, head_grads)
    for bit in range(local_levels):
        parts = joined(
            parts,
            jax.tree.map(
                lambda part, own: part.astype(own.dtype),
                partner(shortened(parts), "seq", bit),
                parts,
            ),
            bit,
        )
    group_query, group_grad = parts
    parts = (row_max, row_sum, row_delta)
    for bit in range(local_levels):
        parts = joined(parts, partner(parts, "seq", bit), bit)
    group_max, group_sum, group_delta = parts
    back_scores = masked(group_query, head_keys, 0, local_rank * tokens, factor)
    back_prob, back_dscore = score_grads(
        back_scores, group_max, group_sum, group_grad, head_values, group_delta
    )
    key_grad = product(back_dscore, group_query, "hij,hid->hjd") * factor
    value_grad = product(back_prob, group_grad, "hij,hid->hjd")
    pair_grad = select(head_grads, 2, pair_branch_shift)
    pair_max = select(row_max, 2, pair_branch_shift)
    pair_sum = select(row_sum, 2, pair_branch_shift)
    pair_delta = select(row_delta, 2, pair_branch_shift)
    _, pair_dscore = score_grads(
        pair_scores, pair_max, pair_sum, pair_grad, pair_all_value, pair_delta
    )
    pair_dq = product(pair_dscore, pair_all_key, "hij,hjd->hid") * factor
    near_rows = (
        select(group_query, 2, pair_branch_shift),
        select(group_grad, 2, pair_branch_shift),
    )
    near_moments = (
        select(group_max, 2, pair_branch_shift),
        select(group_sum, 2, pair_branch_shift),
        select(group_delta, 2, pair_branch_shift),
    )
    all_query, all_grad = joined(
        near_rows, partner((near_rows[0], near_rows[1]), "seq", local_levels), local_levels
    )
    all_max, all_sum, all_delta = joined(
        near_moments,
        partner((near_moments[0], near_moments[1], near_moments[2]), "seq", local_levels),
        local_levels,
    )
    pair_back = masked(all_query, pair_key, 0, pair_rank * half_rows, factor)
    pair_back_prob, pair_back_dscore = score_grads(
        pair_back, all_max, all_sum, all_grad, pair_value, all_delta
    )
    pair_dk = product(pair_back_dscore, all_query, "hij,hid->hjd") * factor
    pair_dv = product(pair_back_prob, all_grad, "hij,hid->hjd")
    query_grad = query_grad + spread(pair_dq, 2, pair_branch_shift, 0.0)
    key_grad = key_grad + spread(pair_dk, 2, pair_branch_shift, 0.0)
    value_grad = value_grad + spread(pair_dv, 2, pair_branch_shift, 0.0)
    far_grad = select(head_grads, dilation, far_branch_shift)
    far_max = select(row_max, dilation, far_branch_shift)
    far_sum = select(row_sum, dilation, far_branch_shift)
    far_delta = select(row_delta, dilation, far_branch_shift)
    far_prob, far_dscore = score_grads(
        far_scores, far_max, far_sum, far_grad, every_value, far_delta
    )
    far_dq = product(far_dscore, every_key, "hij,hjd->hid") * factor
    gathered_dk = product(far_dscore, far_query, "hij,hid->hjd") * factor
    gathered_dv = product(far_prob, far_grad, "hij,hid->hjd")
    far_dk, far_dv = (
        lax.psum_scatter(gathered_dk, "seq", scatter_dimension=1, tiled=True),
        lax.psum_scatter(gathered_dv, "seq", scatter_dimension=1, tiled=True),
    )
    query_grad = query_grad + spread(far_dq, dilation, far_branch_shift, 0.0)
    key_grad = key_grad + spread(far_dk, dilation, far_branch_shift, 0.0)
    value_grad = value_grad + spread(far_dv, dilation, far_branch_shift, 0.0)
    return (
        layer_out,
        by_token(query_grad).astype(jnp.bfloat16),
        by_token(key_grad).astype(jnp.bfloat16),
        by_token(value_grad).astype(jnp.bfloat16),
    )


def lanes(index):
    return pl.ds(pl.multiple_of(index * HEAD_DIM, HEAD_DIM), HEAD_DIM)


def rows(index, length):
    return pl.ds(pl.multiple_of(index * length, length), length)


def matmul(left, right, dims):
    return lax.dot_general(left, right, (dims, ((), ())), preferred_element_type=jnp.float32)


NN = ((1,), (0,))
NT = ((1,), (1,))
TN = ((0,), (0,))


def call(body, out_shape, in_specs, scratch=(), flops=0):
    vmem = pl.BlockSpec(memory_space=pltpu.VMEM)
    return pl.pallas_call(
        body,
        out_shape=out_shape,
        in_specs=in_specs,
        out_specs=jax.tree.map(lambda _: vmem, out_shape),
        scratch_shapes=list(scratch),
        cost_estimate=pl.CostEstimate(flops=flops, bytes_accessed=0, transcendentals=0),
        compiler_params=pltpu.CompilerParams(vmem_limit_bytes=40 * 2**20),
    )


def fast_local(plan, queries, key_rows, value_rows, out_weight, grad_out, pair_offsets, far_offsets):
    tokens, heads, group, selected, dilation, head_groups = plan
    factor = HEAD_DIM ** (-0.5)
    width = heads * HEAD_DIM
    model = out_weight.shape[1]
    span = group * tokens
    far_rows = tokens // dilation
    far_span = span // dilation
    bf16, f32 = jnp.bfloat16, jnp.float32
    vmem = pl.BlockSpec(memory_space=pltpu.VMEM)
    smem = pl.BlockSpec(memory_space=pltpu.SMEM)
    dests = range(group)

    def shape(extent, dtype=bf16):
        return jax.ShapeDtypeStruct(extent, dtype)

    def seq_rank():
        return lax.rem(lax.axis_index("seq"), group)

    def late_half():
        return lax.axis_index("seq") // group

    def my_head():
        return lax.axis_index("head") * heads + seq_rank()

    def swap(value, axis, mask):
        return lax.ppermute(value, axis, [(s, s ^ mask) for s in range(lax.axis_size(axis))])

    def swapped(blocks):
        return [blocks[0]] + [swap(blocks[m], "seq", m) for m in dests if m]

    grads = [grad_out] + [swap(grad_out, "head", m) for m in range(1, head_groups)]

    def pack(fo, q, k, v, *refs):
        outs, fars, wide = refs[:group], refs[group : 2 * group], refs[2 * group :]
        rank = seq_rank()
        base = lax.axis_index("head") * heads
        for m in dests:
            head = rank ^ m
            key, value = k[:, lanes(head)], v[:, lanes(head)]
            outs[m][:, :HEAD_DIM] = q[:, lanes(head)]
            outs[m][:, HEAD_DIM : 2 * HEAD_DIM] = key
            outs[m][:, 2 * HEAD_DIM :] = value
            at = pl.ds(fo[base + head], far_rows, stride=dilation)
            for slot, part in enumerate((key, value)):
                wide[slot][...] = part.astype(f32)
                cols = slice(slot * HEAD_DIM, (slot + 1) * HEAD_DIM)
                fars[m][:, cols] = wide[slot][at, :].astype(bf16)

    packed = call(
        pack,
        [shape((tokens, 3 * HEAD_DIM))] * group + [shape((far_rows, 2 * HEAD_DIM))] * group,
        [smem, vmem, vmem, vmem],
        [pltpu.VMEM((tokens, HEAD_DIM), f32)] * 2,
        flops=10**7,
    )(far_offsets, queries, key_rows, value_rows)
    blocks = swapped(packed[:group])
    early = [
        lax.ppermute(packed[group + m], "seq", [(s, group + (s ^ m)) for s in range(group)])
        for m in dests
    ]

    def project_grad(w, *refs):
        parts, outs, (acc,) = refs[:head_groups], refs[head_groups:-1], refs[-1:]
        me = lax.axis_index("head")
        for m in range(head_groups):
            cols = pl.ds(pl.multiple_of((me ^ m) * width, width), width)
            term = matmul(parts[m][...], w[:, cols], NT)
            if m == 0:
                acc[...] = term
            else:
                acc[...] += term
        rank = seq_rank()
        for m in dests:
            outs[m][...] = acc[:, lanes(rank ^ m)].astype(bf16)

    grad_blocks = swapped(
        call(
            project_grad,
            [shape((tokens, HEAD_DIM))] * group,
            [vmem] * (1 + head_groups),
            [pltpu.VMEM((tokens, width), f32)],
            flops=10**8,
        )(out_weight, *grads),
    )

    def branch_scores(query, key, mask):
        return jnp.where(mask, matmul(query, key, NT) * factor, masked_score)

    def causal(extent, shift=0):
        row_ids = lax.broadcasted_iota(jnp.int32, extent, 0)
        col_ids = lax.broadcasted_iota(jnp.int32, extent, 1)
        return row_ids + shift >= col_ids

    def far_mask():
        extent = (far_span, 2 * far_span)
        col_ids = lax.broadcasted_iota(jnp.int32, extent, 1)
        open_cols = jnp.where(late_half() > 0, 0, far_span)
        return causal(extent, far_span) & (col_ids >= open_cols)

    def stats(scores, value):
        top = jnp.max(scores, axis=-1, keepdims=True)
        weights = jnp.exp(scores - top)
        total = jnp.sum(weights, axis=-1, keepdims=True)
        return top, total, matmul(weights.astype(bf16), value, NN)

    def spread_lanes(column):
        return jnp.broadcast_to(column, (column.shape[0], HEAD_DIM))

    def forward(po, fo, *refs):
        parts, fars = refs[:group], refs[group : 2 * group]
        refs = refs[2 * group :]
        outs, refs = refs[:group], refs[group:]
        out_wide, lse, qb, kb, vb, early_kv, qf, kf, vf, top_all, sum_all = refs
        rank = seq_rank()
        for m in dests:
            at = rows(rank ^ m, tokens)
            for slot, (narrow, wide) in enumerate(((qb, qf), (kb, kf), (vb, vf))):
                part = parts[m][:, slot * HEAD_DIM : (slot + 1) * HEAD_DIM]
                narrow[at, :] = part
                wide[at, :] = part.astype(f32)
            early_kv[rows(rank ^ m, far_rows), :] = fars[m][...]
        pair_at = pl.ds(po[my_head()], selected, stride=2)
        far_at = pl.ds(fo[my_head()], far_span, stride=dilation)
        mask = causal((selected, selected))
        results = []
        for first in range(0, span, selected):
            at = pl.ds(first, selected)
            results.append((at, stats(branch_scores(qb[at, :], kb[at, :], mask), vb[at, :])))
        pick = lambda ref, at: ref[at, :].astype(bf16)
        results.append(
            (
                pair_at,
                stats(
                    branch_scores(pick(qf, pair_at), pick(kf, pair_at), mask), pick(vf, pair_at)
                ),
            )
        )
        far_key = jnp.concatenate([early_kv[:, :HEAD_DIM], pick(kf, far_at)], axis=0)
        far_value = jnp.concatenate([early_kv[:, HEAD_DIM:], pick(vf, far_at)], axis=0)
        results.append(
            (far_at, stats(branch_scores(pick(qf, far_at), far_key, far_mask()), far_value))
        )
        first_part = span // selected
        for number, (at, (top, _, _)) in enumerate(results):
            if number < first_part:
                top_all[at, :] = spread_lanes(top)
            else:
                top_all[at, :] = jnp.maximum(top_all[at, :], spread_lanes(top))
        for number, (at, (top, total, numerator)) in enumerate(results):
            scale = jnp.exp(top - top_all[at, :])
            if number < first_part:
                sum_all[at, :] = total * scale
                out_wide[at, :] = numerator * scale
            else:
                sum_all[at, :] += total * scale
                out_wide[at, :] += numerator * scale
        out_wide[...] = out_wide[...] / sum_all[...]
        lse[...] = top_all[...] + jnp.log(sum_all[...])
        for m in dests:
            outs[m][...] = out_wide[rows(rank ^ m, tokens), :].astype(bf16)

    wide = shape((span, HEAD_DIM), f32)
    narrow = shape((span, HEAD_DIM))
    scratch = pltpu.VMEM((span, HEAD_DIM), f32)
    forward_out = call(
        forward,
        [shape((tokens, HEAD_DIM))] * group
        + [wide, wide, narrow, narrow, narrow, shape((far_span, 2 * HEAD_DIM))],
        [smem, smem] + [vmem] * (2 * group),
        [scratch] * 5,
        flops=3 * 10**8,
    )(pair_offsets, far_offsets, *blocks, *early)
    attended = swapped(forward_out[:group])

    def backward(po, fo, out_wide, lse, qb, kb, vb, early_kv, *refs):
        parts, refs = refs[:group], refs[group:]
        outs, fars, refs = refs[:group], refs[group : 2 * group], refs[2 * group :]
        qf, kf, vf, gf, gb, delta, dq, dk, dv, far_kv = refs
        rank = seq_rank()
        for m in dests:
            at = rows(rank ^ m, tokens)
            gb[at, :] = parts[m][...]
            gf[at, :] = parts[m][...].astype(f32)
        qf[...] = qb[...].astype(f32)
        kf[...] = kb[...].astype(f32)
        vf[...] = vb[...].astype(f32)
        delta[...] = spread_lanes(jnp.sum(gf[...] * out_wide[...], axis=-1, keepdims=True))
        pair_at = pl.ds(po[my_head()], selected, stride=2)
        far_at = pl.ds(fo[my_head()], far_span, stride=dilation)

        def grads_of(query, key, value, grad, row_lse, row_delta, mask):
            scores = branch_scores(query, key, mask)
            probability = jnp.exp(scores - row_lse[:, :1])
            prob_grad = matmul(grad, value, NT)
            score_grad = (probability * (prob_grad - row_delta[:, :1])).astype(bf16)
            return (
                matmul(score_grad, key, NN) * factor,
                matmul(score_grad, query, TN) * factor,
                matmul(probability.astype(bf16), grad, TN),
            )

        mask = causal((selected, selected))
        for first in range(0, span, selected):
            at = pl.ds(first, selected)
            dq[at, :], dk[at, :], dv[at, :] = grads_of(
                qb[at, :], kb[at, :], vb[at, :], gb[at, :], lse[at, :], delta[at, :], mask
            )
        pick = lambda ref, at: ref[at, :].astype(bf16)
        pair_dq, pair_dk, pair_dv = grads_of(
            pick(qf, pair_at),
            pick(kf, pair_at),
            pick(vf, pair_at),
            pick(gf, pair_at),
            lse[pair_at, :],
            delta[pair_at, :],
            mask,
        )
        dq[pair_at, :] += pair_dq
        dk[pair_at, :] += pair_dk
        dv[pair_at, :] += pair_dv
        far_dq, far_dk, far_dv = grads_of(
            pick(qf, far_at),
            jnp.concatenate([early_kv[:, :HEAD_DIM], pick(kf, far_at)], axis=0),
            jnp.concatenate([early_kv[:, HEAD_DIM:], pick(vf, far_at)], axis=0),
            pick(gf, far_at),
            lse[far_at, :],
            delta[far_at, :],
            far_mask(),
        )
        dq[far_at, :] += far_dq
        dk[far_at, :] += far_dk[far_span:]
        dv[far_at, :] += far_dv[far_span:]
        far_kv[:, :HEAD_DIM] = far_dk[:far_span].astype(bf16)
        far_kv[:, HEAD_DIM:] = far_dv[:far_span].astype(bf16)
        for m in dests:
            at = rows(rank ^ m, tokens)
            for slot, ref in enumerate((dq, dk, dv)):
                outs[m][:, slot * HEAD_DIM : (slot + 1) * HEAD_DIM] = ref[at, :].astype(bf16)
            fars[m][...] = far_kv[rows(rank ^ m, far_rows), :]

    backward_out = call(
        backward,
        [shape((tokens, 3 * HEAD_DIM))] * group + [shape((far_rows, 2 * HEAD_DIM))] * group,
        [smem, smem] + [vmem] * (6 + group),
        [scratch] * 4
        + [pltpu.VMEM((span, HEAD_DIM), bf16)]
        + [scratch] * 4
        + [pltpu.VMEM((far_span, 2 * HEAD_DIM), bf16)],
        flops=6 * 10**8,
    )(pair_offsets, far_offsets, *forward_out[group:], *grad_blocks)
    returned = swapped(backward_out[:group])
    late = [
        lax.ppermute(backward_out[group + m], "seq", [(group + s, s ^ m) for s in range(group)])
        for m in dests
    ]

    half = model // 2

    def columns(bit):
        return pl.ds(pl.multiple_of(bit * half, half), half)

    def my_half():
        return lax.rem(lax.axis_index("head"), 2)

    def project_theirs(w, *refs):
        parts, (both, send) = refs[:group], refs[group:]
        rank = seq_rank()
        for m in dests:
            both[:, lanes(rank ^ m)] = parts[m][...]
        send[...] = matmul(both[...], w[:, columns(1 - my_half())], NN).astype(bf16)

    both, theirs = call(
        project_theirs,
        [shape((tokens, width)), shape((tokens, half))],
        [vmem] * (1 + group),
        flops=10**8,
    )(out_weight, *attended)
    mate = swap(theirs, "head", 1)

    def project_mine(w, both, mate, out):
        mine = matmul(both[...], w[:, columns(my_half())], NN).astype(bf16).astype(f32)
        out[...] = (mine + mate[...].astype(f32)).astype(bf16)

    pair_sum = call(project_mine, shape((tokens, half)), [vmem] * 3, flops=10**8)(
        out_weight, both, mate
    )
    across = swap(pair_sum, "head", 2)

    def add(first, second, out):
        out[...] = (first[...].astype(f32) + second[...].astype(f32)).astype(bf16)

    total = call(add, shape((tokens, half)), [vmem] * 2, flops=10**6)(pair_sum, across)
    other = swap(total, "head", 1)

    def join(mine, theirs, out):
        out[:, columns(my_half())] = mine[...]
        out[:, columns(1 - my_half())] = theirs[...]

    layer_out = call(join, shape((tokens, model)), [vmem] * 2, flops=10**6)(total, other)

    def collect(fo, *refs):
        parts, fars = refs[:group], refs[group : 2 * group]
        outs, wide = refs[2 * group : 2 * group + 3], refs[2 * group + 3 :]
        rank = seq_rank()
        base = lax.axis_index("head") * heads
        for m in dests:
            head = rank ^ m
            outs[0][:, lanes(head)] = parts[m][:, :HEAD_DIM]
            at = pl.ds(fo[base + head], far_rows, stride=dilation)
            for slot in range(2):
                cols = slice((slot + 1) * HEAD_DIM, (slot + 2) * HEAD_DIM)
                far_cols = slice(slot * HEAD_DIM, (slot + 1) * HEAD_DIM)
                wide[slot][...] = parts[m][:, cols].astype(f32)
                wide[slot][at, :] += fars[m][:, far_cols].astype(f32)
                outs[1 + slot][:, lanes(head)] = wide[slot][...].astype(bf16)

    gradients = call(
        collect,
        [shape((tokens, width))] * 3,
        [smem] + [vmem] * (2 * group),
        [pltpu.VMEM((tokens, HEAD_DIM), f32)] * 2,
        flops=10**7,
    )(far_offsets, *returned, *late)
    return (layer_out, *gradients)


def local(queries, key_rows, value_rows, out_weight, grad_out, pair_offsets, far_head_offsets):
    tokens = queries.shape[0]
    heads = queries.shape[1] // HEAD_DIM
    seq_count = lax.axis_size("seq")
    total = tokens * seq_count
    selected = min(SPAN, total // 4)
    group = 2 * selected // tokens
    operands = (
        queries, key_rows, value_rows, out_weight, grad_out, pair_offsets, far_head_offsets
    )
    if group == heads and seq_count == 2 * group and lax.axis_size("head") == 4:
        plan = (tokens, heads, group, selected, total // selected, lax.axis_size("head"))
        return fast_local(plan, *operands)
    return exchange_local(*operands)


def solution(mesh):
    placed = (
        P("seq", "head"),
        P("seq", "head"),
        P("seq", "head"),
        P("head", None),
        P("seq", "head"),
        P(),
        P(),
    )
    return jax.shard_map(
        local,
        mesh=mesh,
        in_specs=placed,
        out_specs=(P("seq", None), P("seq", "head"), P("seq", "head"), P("seq", "head")),
        check_vma=False,
    )
```

```python
import jax
import jax.numpy as jnp
from jax import lax
from jax.experimental import pallas as pl
from jax.experimental.pallas import tpu as pltpu
from jax.sharding import PartitionSpec as P

HEAD_DIM = 128
SPAN = 512


masked_score = -1e30


def shortened(array):
    return jax.tree.map(lambda a: a.astype(jnp.bfloat16) if a.dtype == jnp.float32 else a, array)


def partner(value, axis, distance):
    mask = 2**distance
    pairs = [(source, source ^ mask) for source in range(lax.axis_size(axis))]
    return lax.ppermute(value, axis, pairs)


def select(tensor, token_stride, start_offset):
    head_count = tensor.shape[0]
    number = tensor.shape[1] // token_stride
    shaped = tensor.reshape((head_count, number, token_stride) + tensor.shape[2:])
    lane_ids = lax.broadcasted_iota(jnp.int32, shaped.shape, 2)
    chosen = start_offset.reshape((head_count, 1, 1) + (1,) * (tensor.ndim - 2))
    return jnp.sum(jnp.where(lane_ids == chosen, shaped, jnp.zeros((), tensor.dtype)), axis=2)


def spread(entries, token_stride, start_offset, filler):
    head_count = entries.shape[0]
    number = entries.shape[1]
    layout = (head_count, number, token_stride) + entries.shape[2:]
    lane_ids = lax.broadcasted_iota(jnp.int32, layout, 2)
    chosen = start_offset.reshape((head_count, 1, 1) + (1,) * (entries.ndim - 2))
    placed = jnp.where(lane_ids == chosen, jnp.expand_dims(entries, 2), filler)
    return placed.reshape((head_count, number * token_stride) + entries.shape[2:])


def product(left_side, right_side, pattern):
    return jnp.einsum(pattern, left_side, right_side, preferred_element_type=jnp.float32)


def masked(query_part, key_part, first_row, first_col, factor):
    scores = product(query_part, key_part, "hid,hjd->hij") * factor
    row_ids = first_row + lax.broadcasted_iota(jnp.int32, scores.shape, 1)
    col_ids = first_col + lax.broadcasted_iota(jnp.int32, scores.shape, 2)
    return jnp.where(row_ids >= col_ids, scores, masked_score)


def branch_stats(scores, value_part):
    branch_max = jnp.max(scores, axis=-1)
    weights = jnp.exp(scores - branch_max[..., None])
    numerator = product(weights.astype(jnp.bfloat16), value_part, "hij,hjd->hid")
    return (branch_max, jnp.sum(weights, axis=-1), numerator)


def score_grads(scores, row_max, row_sum, grad_part, value_part, row_delta):
    probability = jnp.exp(scores - row_max[..., None]) / row_sum[..., None]
    prob_grad = product(grad_part, value_part, "hid,hjd->hij")
    score_grad = (probability * (prob_grad - row_delta[..., None])).astype(jnp.bfloat16)
    return (probability.astype(jnp.bfloat16), score_grad)


def exchange_local(queries, key_rows, value_rows, out_weight, grad_out, pair_offsets, far_head_offsets):
    tokens = queries.shape[0]
    head_count = queries.shape[1] // HEAD_DIM
    factor = HEAD_DIM ** (-0.5)
    seq_count = lax.axis_size("seq")
    total = tokens * seq_count
    selected = min(SPAN, total // 4)
    local_group = selected // tokens
    local_levels = local_group.bit_length() - 1
    dilation = total // selected
    far_rows = tokens // dilation
    half_rows = tokens // 2
    position = lax.axis_index("seq")
    local_rank = position % local_group
    pair_rank = position % (2 * local_group)
    head_group = lax.axis_index("head")
    pair_branch_shift = lax.dynamic_slice_in_dim(pair_offsets, head_group * head_count, head_count)
    far_branch_shift = lax.dynamic_slice_in_dim(
        far_head_offsets, head_group * head_count, head_count
    )

    def by_head(tensor):
        return tensor.reshape(tokens, head_count, HEAD_DIM).transpose(1, 0, 2)

    def by_token(tensor):
        return tensor.transpose(1, 0, 2).reshape(tokens, head_count * HEAD_DIM)

    def stacked(mine, theirs, bit):
        high = position // 2**bit % 2 == 1
        lower = jnp.where(high, theirs, mine)
        upper = jnp.where(high, mine, theirs)
        return jnp.concatenate([lower, upper], axis=1)

    def joined(mine, theirs, bit):
        return tuple((stacked(first, second, bit) for first, second in zip(mine, theirs)))

    head_queries = by_head(queries)
    head_keys = by_head(key_rows)
    head_values = by_head(value_rows)
    parts = (head_keys, head_values)
    for bit in range(local_levels):
        parts = joined(
            parts,
            jax.tree.map(
                lambda part, own: part.astype(own.dtype),
                partner(shortened(parts), "seq", bit),
                parts,
            ),
            bit,
        )
    segment_key, segment_value = parts
    local_scores = masked(head_queries, segment_key, local_rank * tokens, 0, factor)
    local_stats = branch_stats(local_scores, segment_value)
    pair_query = select(head_queries, 2, pair_branch_shift)
    pair_key = select(head_keys, 2, pair_branch_shift)
    pair_value = select(head_values, 2, pair_branch_shift)
    nearby = (
        select(segment_key, 2, pair_branch_shift),
        select(segment_value, 2, pair_branch_shift),
    )
    pair_all_key, pair_all_value = joined(
        nearby, partner((nearby[0], nearby[1]), "seq", local_levels), local_levels
    )
    pair_scores = masked(pair_query, pair_all_key, pair_rank * half_rows, 0, factor)
    pair_stats = branch_stats(pair_scores, pair_all_value)
    far_query = select(head_queries, dilation, far_branch_shift)
    far_key = select(head_keys, dilation, far_branch_shift)
    far_value = select(head_values, dilation, far_branch_shift)
    every_key, every_value = (
        lax.all_gather(far_key, "seq", axis=1, tiled=True),
        lax.all_gather(far_value, "seq", axis=1, tiled=True),
    )
    far_scores = masked(far_query, every_key, position * far_rows, 0, factor)
    far_stats = branch_stats(far_scores, every_value)
    pair_spread = (
        spread(pair_stats[0], 2, pair_branch_shift, masked_score),
        spread(pair_stats[1], 2, pair_branch_shift, 0.0),
        spread(pair_stats[2], 2, pair_branch_shift, 0.0),
    )
    far_spread = (
        spread(far_stats[0], dilation, far_branch_shift, masked_score),
        spread(far_stats[1], dilation, far_branch_shift, 0.0),
        spread(far_stats[2], dilation, far_branch_shift, 0.0),
    )
    row_max = jnp.maximum(jnp.maximum(local_stats[0], pair_spread[0]), far_spread[0])
    row_sum = jnp.zeros_like(row_max)
    numerator = jnp.zeros_like(local_stats[2])
    for branch in (local_stats, pair_spread, far_spread):
        rescale = jnp.exp(branch[0] - row_max)
        row_sum = row_sum + branch[1] * rescale
        numerator = numerator + branch[2] * rescale[..., None]
    head_out = numerator / row_sum[..., None]
    attended = by_token(head_out).astype(jnp.bfloat16)
    partial_out = jnp.dot(attended, out_weight, preferred_element_type=jnp.float32)
    layer_out = lax.psum(partial_out.astype(jnp.bfloat16), "head")
    grad_attended = lax.dot_general(
        lax.all_gather(grad_out, "head", axis=1, tiled=True),
        out_weight,
        (((1,), (1,)), ((), ())),
        preferred_element_type=jnp.float32,
    )
    head_grads = by_head(grad_attended.astype(jnp.bfloat16))
    row_delta = jnp.sum(head_grads.astype(jnp.float32) * head_out, axis=-1)
    _, local_dscore = score_grads(
        local_scores, row_max, row_sum, head_grads, segment_value, row_delta
    )
    query_grad = product(local_dscore, segment_key, "hij,hjd->hid") * factor
    parts = (head_queries, head_grads)
    for bit in range(local_levels):
        parts = joined(
            parts,
            jax.tree.map(
                lambda part, own: part.astype(own.dtype),
                partner(shortened(parts), "seq", bit),
                parts,
            ),
            bit,
        )
    group_query, group_grad = parts
    parts = (row_max, row_sum, row_delta)
    for bit in range(local_levels):
        parts = joined(parts, partner(parts, "seq", bit), bit)
    group_max, group_sum, group_delta = parts
    back_scores = masked(group_query, head_keys, 0, local_rank * tokens, factor)
    back_prob, back_dscore = score_grads(
        back_scores, group_max, group_sum, group_grad, head_values, group_delta
    )
    key_grad = product(back_dscore, group_query, "hij,hid->hjd") * factor
    value_grad = product(back_prob, group_grad, "hij,hid->hjd")
    pair_grad = select(head_grads, 2, pair_branch_shift)
    pair_max = select(row_max, 2, pair_branch_shift)
    pair_sum = select(row_sum, 2, pair_branch_shift)
    pair_delta = select(row_delta, 2, pair_branch_shift)
    _, pair_dscore = score_grads(
        pair_scores, pair_max, pair_sum, pair_grad, pair_all_value, pair_delta
    )
    pair_dq = product(pair_dscore, pair_all_key, "hij,hjd->hid") * factor
    near_rows = (
        select(group_query, 2, pair_branch_shift),
        select(group_grad, 2, pair_branch_shift),
    )
    near_moments = (
        select(group_max, 2, pair_branch_shift),
        select(group_sum, 2, pair_branch_shift),
        select(group_delta, 2, pair_branch_shift),
    )
    all_query, all_grad = joined(
        near_rows, partner((near_rows[0], near_rows[1]), "seq", local_levels), local_levels
    )
    all_max, all_sum, all_delta = joined(
        near_moments,
        partner((near_moments[0], near_moments[1], near_moments[2]), "seq", local_levels),
        local_levels,
    )
    pair_back = masked(all_query, pair_key, 0, pair_rank * half_rows, factor)
    pair_back_prob, pair_back_dscore = score_grads(
        pair_back, all_max, all_sum, all_grad, pair_value, all_delta
    )
    pair_dk = product(pair_back_dscore, all_query, "hij,hid->hjd") * factor
    pair_dv = product(pair_back_prob, all_grad, "hij,hid->hjd")
    query_grad = query_grad + spread(pair_dq, 2, pair_branch_shift, 0.0)
    key_grad = key_grad + spread(pair_dk, 2, pair_branch_shift, 0.0)
    value_grad = value_grad + spread(pair_dv, 2, pair_branch_shift, 0.0)
    far_grad = select(head_grads, dilation, far_branch_shift)
    far_max = select(row_max, dilation, far_branch_shift)
    far_sum = select(row_sum, dilation, far_branch_shift)
    far_delta = select(row_delta, dilation, far_branch_shift)
    far_prob, far_dscore = score_grads(
        far_scores, far_max, far_sum, far_grad, every_value, far_delta
    )
    far_dq = product(far_dscore, every_key, "hij,hjd->hid") * factor
    gathered_dk = product(far_dscore, far_query, "hij,hid->hjd") * factor
    gathered_dv = product(far_prob, far_grad, "hij,hid->hjd")
    far_dk, far_dv = (
        lax.psum_scatter(gathered_dk, "seq", scatter_dimension=1, tiled=True),
        lax.psum_scatter(gathered_dv, "seq", scatter_dimension=1, tiled=True),
    )
    query_grad = query_grad + spread(far_dq, dilation, far_branch_shift, 0.0)
    key_grad = key_grad + spread(far_dk, dilation, far_branch_shift, 0.0)
    value_grad = value_grad + spread(far_dv, dilation, far_branch_shift, 0.0)
    return (
        layer_out,
        by_token(query_grad).astype(jnp.bfloat16),
        by_token(key_grad).astype(jnp.bfloat16),
        by_token(value_grad).astype(jnp.bfloat16),
    )


def lanes(index):
    return pl.ds(pl.multiple_of(index * HEAD_DIM, HEAD_DIM), HEAD_DIM)


def rows(index, length):
    return pl.ds(pl.multiple_of(index * length, length), length)


def matmul(left, right, dims):
    return lax.dot_general(left, right, (dims, ((), ())), preferred_element_type=jnp.float32)


NN = ((1,), (0,))
NT = ((1,), (1,))
TN = ((0,), (0,))


def call(body, out_shape, in_specs, scratch=(), flops=0, out_space=pltpu.VMEM, limit=40):
    out_spec = pl.BlockSpec(memory_space=out_space)
    return pl.pallas_call(
        body,
        out_shape=out_shape,
        in_specs=in_specs,
        out_specs=jax.tree.map(lambda _: out_spec, out_shape),
        scratch_shapes=list(scratch),
        cost_estimate=pl.CostEstimate(flops=flops, bytes_accessed=0, transcendentals=0),
        compiler_params=pltpu.CompilerParams(vmem_limit_bytes=limit * 2**20 if limit else None),
    )


def fast_local(plan, queries, key_rows, value_rows, out_weight, grad_out, pair_offsets, far_offsets):
    tokens, heads, group, selected, dilation, head_groups = plan
    factor = HEAD_DIM ** (-0.5)
    width = heads * HEAD_DIM
    model = out_weight.shape[1]
    span = group * tokens
    far_span = span // dilation
    bf16, f32 = jnp.bfloat16, jnp.float32
    vmem = pl.BlockSpec(memory_space=pltpu.VMEM)
    smem = pl.BlockSpec(memory_space=pltpu.SMEM)
    dests = range(group)

    def shape(extent, dtype=bf16):
        return jax.ShapeDtypeStruct(extent, dtype)

    def seq_rank():
        return lax.rem(lax.axis_index("seq"), group)

    def late_half():
        return lax.axis_index("seq") // group

    def my_head():
        return lax.axis_index("head") * heads + seq_rank()

    def swap(value, axis, mask):
        pairs = [(s, s ^ mask) for s in range(lax.axis_size(axis))]
        return lax.ppermute(value, axis, pairs)

    def swapped(blocks):
        return [blocks[0]] + [swap(blocks[m], "seq", m) for m in dests if m]

    others = [swap(grad_out, "head", m) for m in range(1, head_groups)]

    def opening(out):
        out[...] = jnp.zeros_like(out)

    opened = call(opening, shape((8, HEAD_DIM), f32), [], flops=2 * 10**10)()

    def pack(opened, q, k, v, *outs):
        rank = seq_rank()
        for slot, ref in enumerate((q, k, v)):
            for m in dests:
                outs[m][:, slot * HEAD_DIM : (slot + 1) * HEAD_DIM] = ref[:, lanes(rank ^ m)]

    packed = call(
        pack, [shape((tokens, 3 * HEAD_DIM))] * group, [vmem] * 4, flops=10**9
    )(opened, queries, key_rows, value_rows)
    blocks = swapped(packed)

    def project_grad(w, *refs):
        parts, outs, (acc,) = refs[:head_groups], refs[head_groups:-1], refs[-1:]
        me = lax.axis_index("head")
        for m in range(head_groups):
            cols = pl.ds(pl.multiple_of((me ^ m) * width, width), width)
            term = matmul(parts[m][...], w[:, cols], NT)
            if m == 0:
                acc[...] = term
            else:
                acc[...] += term
        rank = seq_rank()
        for m in dests:
            outs[m][...] = acc[:, lanes(rank ^ m)].astype(bf16)

    grad_blocks = swapped(
        call(
            project_grad,
            [shape((tokens, HEAD_DIM))] * group,
            [vmem] * (1 + head_groups),
            [pltpu.VMEM((tokens, width), f32)],
            flops=10**8,
        )(out_weight, grad_out, *others),
    )

    def branch_scores(query, key, mask):
        return jnp.where(mask, matmul(query, key, NT) * factor, masked_score)

    def causal(extent, shift=0):
        row_ids = lax.broadcasted_iota(jnp.int32, extent, 0)
        col_ids = lax.broadcasted_iota(jnp.int32, extent, 1)
        return row_ids + shift >= col_ids

    def far_mask():
        extent = (far_span, 2 * far_span)
        col_ids = lax.broadcasted_iota(jnp.int32, extent, 1)
        open_cols = jnp.where(late_half() > 0, 0, far_span)
        return causal(extent, far_span) & (col_ids >= open_cols)

    def stats(scores, value):
        top = jnp.max(scores, axis=-1, keepdims=True)
        weights = jnp.exp(scores - top)
        total = jnp.sum(weights, axis=-1, keepdims=True)
        return top, total, matmul(weights.astype(bf16), value, NN)

    def spread_lanes(column):
        return jnp.broadcast_to(column, (column.shape[0], HEAD_DIM))

    def pick(ref, at):
        return ref[at, :].astype(bf16)

    def pair_rows(po):
        return pl.ds(po[my_head()], selected, stride=2)

    def far_rows(fo):
        return pl.ds(fo[my_head()], far_span, stride=dilation)

    def with_early(early_kv, slot, ref, at):
        cols = slice(slot * HEAD_DIM, (slot + 1) * HEAD_DIM)
        return jnp.concatenate([early_kv[:, cols], pick(ref, at)], axis=0)

    wide = shape((span, HEAD_DIM), f32)
    far_pair = shape((far_span, 2 * HEAD_DIM))

    def assemble(fo, *refs):
        parts, (q, k, v, far_kv) = refs[:group], refs[group:]
        rank = seq_rank()
        for m in dests:
            at = rows(rank ^ m, tokens)
            for slot, ref in enumerate((q, k, v)):
                part = parts[m][:, slot * HEAD_DIM : (slot + 1) * HEAD_DIM]
                ref[at, :] = part.astype(f32)
        far_at = far_rows(fo)
        far_kv[:, :HEAD_DIM] = pick(k, far_at)
        far_kv[:, HEAD_DIM:] = pick(v, far_at)

    q, k, v, far_kv = call(
        assemble, [wide] * 3 + [far_pair], [smem] + [vmem] * group, flops=10**7
    )(far_offsets, *blocks)
    early_kv = swap(far_kv, "seq", group)

    def forward_near(po, q, k, v, top_all, sum_all, acc):
        mask = causal((selected, selected))
        for first in range(0, span, selected):
            at = pl.ds(first, selected)
            top, total, numerator = stats(
                branch_scores(pick(q, at), pick(k, at), mask), pick(v, at)
            )
            top_all[at, :] = spread_lanes(top)
            sum_all[at, :] = spread_lanes(total)
            acc[at, :] = numerator
        merge(
            pair_rows(po),
            stats(
                branch_scores(pick(q, pair_rows(po)), pick(k, pair_rows(po)), mask),
                pick(v, pair_rows(po)),
            ),
            (top_all, sum_all, acc),
        )

    def merge(at, branch, totals):
        top, total, numerator = branch
        top_all, sum_all, acc = totals
        old_top = top_all[at, :]
        new_top = jnp.maximum(old_top, spread_lanes(top))
        old_scale, scale = jnp.exp(old_top - new_top), jnp.exp(top - new_top)
        top_all[at, :] = new_top
        sum_all[at, :] = sum_all[at, :] * old_scale + total * scale
        acc[at, :] = acc[at, :] * old_scale + numerator * scale

    near = call(forward_near, [wide] * 3, [smem] + [vmem] * 3, flops=2 * 10**8)(
        pair_offsets, q, k, v
    )

    def forward_far(fo, q, k, v, early_kv, near_top, near_sum, near_acc, *refs):
        outs, (out_wide, lse, top_all, sum_all) = refs[:group], refs[group:]
        far_at = far_rows(fo)
        top_all[...] = near_top[...]
        sum_all[...] = near_sum[...]
        out_wide[...] = near_acc[...]
        key, value = with_early(early_kv, 0, k, far_at), with_early(early_kv, 1, v, far_at)
        branch = stats(branch_scores(pick(q, far_at), key, far_mask()), value)
        merge(far_at, branch, (top_all, sum_all, out_wide))
        out_wide[...] = out_wide[...] / sum_all[...]
        lse[...] = top_all[...] + jnp.log(sum_all[...])
        rank = seq_rank()
        for m in dests:
            outs[m][...] = out_wide[rows(rank ^ m, tokens), :].astype(bf16)

    scratch = pltpu.VMEM((span, HEAD_DIM), f32)
    *out_blocks, out_wide, lse = call(
        forward_far,
        [shape((tokens, HEAD_DIM))] * group + [wide, wide],
        [smem] + [vmem] * 7,
        [scratch] * 2,
        flops=10**8,
    )(far_offsets, q, k, v, early_kv, *near)
    attended = swapped(out_blocks)

    def grads_of(query, key, value, grad, row_lse, row_delta, mask):
        scores = branch_scores(query, key, mask)
        probability = jnp.exp(scores - row_lse[:, :1])
        prob_grad = matmul(grad, value, NT)
        score_grad = (probability * (prob_grad - row_delta[:, :1])).astype(bf16)
        return (
            matmul(score_grad, key, NN) * factor,
            matmul(score_grad, query, TN) * factor,
            matmul(probability.astype(bf16), grad, TN),
        )

    def backward_far(fo, q, k, v, early_kv, out_wide, lse, *refs):
        parts, (grad, delta, far_dq, far_dk, far_dv, far_kv) = refs[:group], refs[group:]
        rank = seq_rank()
        for m in dests:
            grad[rows(rank ^ m, tokens), :] = parts[m][...].astype(f32)
        delta[...] = spread_lanes(jnp.sum(grad[...] * out_wide[...], axis=-1, keepdims=True))
        at = far_rows(fo)
        far_dq[...], dk, dv = grads_of(
            pick(q, at),
            with_early(early_kv, 0, k, at),
            with_early(early_kv, 1, v, at),
            pick(grad, at),
            lse[at, :],
            delta[at, :],
            far_mask(),
        )
        far_kv[:, :HEAD_DIM] = dk[:far_span].astype(bf16)
        far_kv[:, HEAD_DIM:] = dv[:far_span].astype(bf16)
        far_dk[...] = dk[far_span:]
        far_dv[...] = dv[far_span:]

    far_wide = shape((far_span, HEAD_DIM), f32)
    grad, delta, far_dq, far_dk, far_dv, late_kv = call(
        backward_far,
        [wide, wide] + [far_wide] * 3 + [far_pair],
        [smem] + [vmem] * (6 + group),
        flops=2 * 10**8,
    )(far_offsets, q, k, v, early_kv, out_wide, lse, *grad_blocks)
    late = swap(late_kv, "seq", group)

    def backward_near(po, fo, q, k, v, grad, lse, delta, *refs):
        fars, near = refs[:3], refs[3:]
        mask = causal((selected, selected))
        for first in range(0, span, selected):
            at = pl.ds(first, selected)
            terms = grads_of(
                pick(q, at), pick(k, at), pick(v, at), pick(grad, at), lse[at, :], delta[at, :], mask
            )
            for ref, term in zip(near, terms):
                ref[at, :] = term
        at = pair_rows(po)
        terms = grads_of(
            pick(q, at), pick(k, at), pick(v, at), pick(grad, at), lse[at, :], delta[at, :], mask
        )
        for ref, term in zip(near, terms):
            ref[at, :] += term
        for ref, far in zip(near, fars):
            ref[far_rows(fo), :] += far[...]

    dq, dk, dv = call(
        backward_near, [wide] * 3, [smem, smem] + [vmem] * 9, flops=5 * 10**8
    )(pair_offsets, far_offsets, q, k, v, grad, lse, delta, far_dq, far_dk, far_dv)

    def finish(fo, dq, dk, dv, late, *refs):
        outs, sums = refs[:group], refs[group:]
        at = far_rows(fo)
        for slot, (ref, part) in enumerate(zip(sums, (dk, dv))):
            ref[...] = part[...]
            ref[at, :] += late[:, slot * HEAD_DIM : (slot + 1) * HEAD_DIM].astype(f32)
        rank = seq_rank()
        for m in dests:
            for slot, ref in enumerate((dq, *sums)):
                cols = slice(slot * HEAD_DIM, (slot + 1) * HEAD_DIM)
                outs[m][:, cols] = ref[rows(rank ^ m, tokens), :].astype(bf16)

    returned = swapped(
        call(
            finish,
            [shape((tokens, 3 * HEAD_DIM))] * group,
            [smem] + [vmem] * 4,
            [scratch] * 2,
            flops=10**7,
        )(far_offsets, dq, dk, dv, late),
    )

    half = model // 2

    def columns(bit):
        return pl.ds(pl.multiple_of(bit * half, half), half)

    def my_half():
        return lax.rem(lax.axis_index("head"), 2)

    def project_theirs(w, *refs):
        parts, (both, send) = refs[:group], refs[group:]
        rank = seq_rank()
        for m in dests:
            both[:, lanes(rank ^ m)] = parts[m][...]
        send[...] = matmul(both[...], w[:, columns(1 - my_half())], NN).astype(bf16)

    half_out = shape((tokens, half))
    both, theirs = call(
        project_theirs,
        [shape((tokens, width)), half_out],
        [vmem] * (1 + group),
        flops=10**8,
    )(out_weight, *attended)
    mate = swap(theirs, "head", 1)

    def project_mine(w, both, out):
        out[...] = matmul(both[...], w[:, columns(my_half())], NN).astype(bf16)

    def add_mate(first, second, out):
        out[...] = (first[...].astype(f32) + second[...].astype(f32)).astype(bf16)

    def add_across(first, second, out):
        add_mate(first, second, out)

    mine = call(project_mine, half_out, [vmem] * 2, flops=10**8)(out_weight, both)
    pair_sum = call(add_mate, half_out, [vmem] * 2, flops=10**6)(mine, mate)
    across = swap(pair_sum, "head", 2)
    total = call(add_across, half_out, [vmem] * 2, flops=10**6)(pair_sum, across)
    other = swap(total, "head", 1)

    def copy_all(copies):
        for copy in copies:
            copy.start()
        for copy in copies:
            copy.wait()

    def join(mine, theirs, out, sems):
        copy_all(
            [
                pltpu.make_async_copy(mine, out.at[:, columns(my_half())], sems.at[0]),
                pltpu.make_async_copy(theirs, out.at[:, columns(1 - my_half())], sems.at[1]),
            ]
        )

    layer_out = call(
        join,
        shape((tokens, model)),
        [vmem] * 2,
        [pltpu.SemaphoreType.DMA((2,))],
        flops=10**6,
        out_space=pltpu.HBM,
    )(total, other)

    def collect(*refs):
        parts, outs, sems = refs[:group], refs[group : group + 3], refs[-1]
        rank = seq_rank()
        copy_all(
            [
                pltpu.make_async_copy(
                    parts[m].at[:, slot * HEAD_DIM : (slot + 1) * HEAD_DIM],
                    outs[slot].at[:, lanes(rank ^ m)],
                    sems.at[m, slot],
                )
                for m in dests
                for slot in range(3)
            ]
        )

    gradients = call(
        collect,
        [shape((tokens, width))] * 3,
        [vmem] * group,
        [pltpu.SemaphoreType.DMA((group, 3))],
        flops=10**7,
        out_space=pltpu.HBM,
    )(*returned)
    return (layer_out, *gradients)


def local(queries, key_rows, value_rows, out_weight, grad_out, pair_offsets, far_head_offsets):
    tokens = queries.shape[0]
    heads = queries.shape[1] // HEAD_DIM
    seq_count = lax.axis_size("seq")
    total = tokens * seq_count
    selected = min(SPAN, total // 4)
    group = 2 * selected // tokens
    operands = (
        queries, key_rows, value_rows, out_weight, grad_out, pair_offsets, far_head_offsets
    )
    if group == heads and seq_count == 2 * group and lax.axis_size("head") == 4:
        plan = (tokens, heads, group, selected, total // selected, lax.axis_size("head"))
        return fast_local(plan, *operands)
    return exchange_local(*operands)


def solution(mesh):
    placed = (
        P("seq", "head"),
        P("seq", "head"),
        P("seq", "head"),
        P("head", None),
        P("seq", "head"),
        P(),
        P(),
    )
    return jax.shard_map(
        local,
        mesh=mesh,
        in_specs=placed,
        out_specs=(P("seq", None), P("seq", "head"), P("seq", "head"), P("seq", "head")),
        check_vma=False,
    )
```

```python
import jax
import jax.numpy as jnp
from jax import lax
from jax.experimental import pallas as pl
from jax.experimental.pallas import tpu as pltpu
from jax.sharding import PartitionSpec as P

HEAD_DIM = 128
SPAN = 512


masked_score = -1e30


def shortened(array):
    return jax.tree.map(lambda a: a.astype(jnp.bfloat16) if a.dtype == jnp.float32 else a, array)


def partner(value, axis, distance):
    mask = 2**distance
    pairs = [(source, source ^ mask) for source in range(lax.axis_size(axis))]
    return lax.ppermute(value, axis, pairs)


def select(tensor, token_stride, start_offset):
    head_count = tensor.shape[0]
    number = tensor.shape[1] // token_stride
    shaped = tensor.reshape((head_count, number, token_stride) + tensor.shape[2:])
    lane_ids = lax.broadcasted_iota(jnp.int32, shaped.shape, 2)
    chosen = start_offset.reshape((head_count, 1, 1) + (1,) * (tensor.ndim - 2))
    return jnp.sum(jnp.where(lane_ids == chosen, shaped, jnp.zeros((), tensor.dtype)), axis=2)


def spread(entries, token_stride, start_offset, filler):
    head_count = entries.shape[0]
    number = entries.shape[1]
    layout = (head_count, number, token_stride) + entries.shape[2:]
    lane_ids = lax.broadcasted_iota(jnp.int32, layout, 2)
    chosen = start_offset.reshape((head_count, 1, 1) + (1,) * (entries.ndim - 2))
    placed = jnp.where(lane_ids == chosen, jnp.expand_dims(entries, 2), filler)
    return placed.reshape((head_count, number * token_stride) + entries.shape[2:])


def product(left_side, right_side, pattern):
    return jnp.einsum(pattern, left_side, right_side, preferred_element_type=jnp.float32)


def masked(query_part, key_part, first_row, first_col, factor):
    scores = product(query_part, key_part, "hid,hjd->hij") * factor
    row_ids = first_row + lax.broadcasted_iota(jnp.int32, scores.shape, 1)
    col_ids = first_col + lax.broadcasted_iota(jnp.int32, scores.shape, 2)
    return jnp.where(row_ids >= col_ids, scores, masked_score)


def branch_stats(scores, value_part):
    branch_max = jnp.max(scores, axis=-1)
    weights = jnp.exp(scores - branch_max[..., None])
    numerator = product(weights.astype(jnp.bfloat16), value_part, "hij,hjd->hid")
    return (branch_max, jnp.sum(weights, axis=-1), numerator)


def score_grads(scores, row_max, row_sum, grad_part, value_part, row_delta):
    probability = jnp.exp(scores - row_max[..., None]) / row_sum[..., None]
    prob_grad = product(grad_part, value_part, "hid,hjd->hij")
    score_grad = (probability * (prob_grad - row_delta[..., None])).astype(jnp.bfloat16)
    return (probability.astype(jnp.bfloat16), score_grad)


def exchange_local(queries, key_rows, value_rows, out_weight, grad_out, pair_offsets, far_head_offsets):
    tokens = queries.shape[0]
    head_count = queries.shape[1] // HEAD_DIM
    factor = HEAD_DIM ** (-0.5)
    seq_count = lax.axis_size("seq")
    total = tokens * seq_count
    selected = min(SPAN, total // 4)
    local_group = selected // tokens
    local_levels = local_group.bit_length() - 1
    dilation = total // selected
    far_rows = tokens // dilation
    half_rows = tokens // 2
    position = lax.axis_index("seq")
    local_rank = position % local_group
    pair_rank = position % (2 * local_group)
    head_group = lax.axis_index("head")
    pair_branch_shift = lax.dynamic_slice_in_dim(pair_offsets, head_group * head_count, head_count)
    far_branch_shift = lax.dynamic_slice_in_dim(
        far_head_offsets, head_group * head_count, head_count
    )

    def by_head(tensor):
        return tensor.reshape(tokens, head_count, HEAD_DIM).transpose(1, 0, 2)

    def by_token(tensor):
        return tensor.transpose(1, 0, 2).reshape(tokens, head_count * HEAD_DIM)

    def stacked(mine, theirs, bit):
        high = position // 2**bit % 2 == 1
        lower = jnp.where(high, theirs, mine)
        upper = jnp.where(high, mine, theirs)
        return jnp.concatenate([lower, upper], axis=1)

    def joined(mine, theirs, bit):
        return tuple((stacked(first, second, bit) for first, second in zip(mine, theirs)))

    head_queries = by_head(queries)
    head_keys = by_head(key_rows)
    head_values = by_head(value_rows)
    parts = (head_keys, head_values)
    for bit in range(local_levels):
        parts = joined(
            parts,
            jax.tree.map(
                lambda part, own: part.astype(own.dtype),
                partner(shortened(parts), "seq", bit),
                parts,
            ),
            bit,
        )
    segment_key, segment_value = parts
    local_scores = masked(head_queries, segment_key, local_rank * tokens, 0, factor)
    local_stats = branch_stats(local_scores, segment_value)
    pair_query = select(head_queries, 2, pair_branch_shift)
    pair_key = select(head_keys, 2, pair_branch_shift)
    pair_value = select(head_values, 2, pair_branch_shift)
    nearby = (
        select(segment_key, 2, pair_branch_shift),
        select(segment_value, 2, pair_branch_shift),
    )
    pair_all_key, pair_all_value = joined(
        nearby, partner((nearby[0], nearby[1]), "seq", local_levels), local_levels
    )
    pair_scores = masked(pair_query, pair_all_key, pair_rank * half_rows, 0, factor)
    pair_stats = branch_stats(pair_scores, pair_all_value)
    far_query = select(head_queries, dilation, far_branch_shift)
    far_key = select(head_keys, dilation, far_branch_shift)
    far_value = select(head_values, dilation, far_branch_shift)
    every_key, every_value = (
        lax.all_gather(far_key, "seq", axis=1, tiled=True),
        lax.all_gather(far_value, "seq", axis=1, tiled=True),
    )
    far_scores = masked(far_query, every_key, position * far_rows, 0, factor)
    far_stats = branch_stats(far_scores, every_value)
    pair_spread = (
        spread(pair_stats[0], 2, pair_branch_shift, masked_score),
        spread(pair_stats[1], 2, pair_branch_shift, 0.0),
        spread(pair_stats[2], 2, pair_branch_shift, 0.0),
    )
    far_spread = (
        spread(far_stats[0], dilation, far_branch_shift, masked_score),
        spread(far_stats[1], dilation, far_branch_shift, 0.0),
        spread(far_stats[2], dilation, far_branch_shift, 0.0),
    )
    row_max = jnp.maximum(jnp.maximum(local_stats[0], pair_spread[0]), far_spread[0])
    row_sum = jnp.zeros_like(row_max)
    numerator = jnp.zeros_like(local_stats[2])
    for branch in (local_stats, pair_spread, far_spread):
        rescale = jnp.exp(branch[0] - row_max)
        row_sum = row_sum + branch[1] * rescale
        numerator = numerator + branch[2] * rescale[..., None]
    head_out = numerator / row_sum[..., None]
    attended = by_token(head_out).astype(jnp.bfloat16)
    partial_out = jnp.dot(attended, out_weight, preferred_element_type=jnp.float32)
    layer_out = lax.psum(partial_out.astype(jnp.bfloat16), "head")
    grad_attended = lax.dot_general(
        lax.all_gather(grad_out, "head", axis=1, tiled=True),
        out_weight,
        (((1,), (1,)), ((), ())),
        preferred_element_type=jnp.float32,
    )
    head_grads = by_head(grad_attended.astype(jnp.bfloat16))
    row_delta = jnp.sum(head_grads.astype(jnp.float32) * head_out, axis=-1)
    _, local_dscore = score_grads(
        local_scores, row_max, row_sum, head_grads, segment_value, row_delta
    )
    query_grad = product(local_dscore, segment_key, "hij,hjd->hid") * factor
    parts = (head_queries, head_grads)
    for bit in range(local_levels):
        parts = joined(
            parts,
            jax.tree.map(
                lambda part, own: part.astype(own.dtype),
                partner(shortened(parts), "seq", bit),
                parts,
            ),
            bit,
        )
    group_query, group_grad = parts
    parts = (row_max, row_sum, row_delta)
    for bit in range(local_levels):
        parts = joined(parts, partner(parts, "seq", bit), bit)
    group_max, group_sum, group_delta = parts
    back_scores = masked(group_query, head_keys, 0, local_rank * tokens, factor)
    back_prob, back_dscore = score_grads(
        back_scores, group_max, group_sum, group_grad, head_values, group_delta
    )
    key_grad = product(back_dscore, group_query, "hij,hid->hjd") * factor
    value_grad = product(back_prob, group_grad, "hij,hid->hjd")
    pair_grad = select(head_grads, 2, pair_branch_shift)
    pair_max = select(row_max, 2, pair_branch_shift)
    pair_sum = select(row_sum, 2, pair_branch_shift)
    pair_delta = select(row_delta, 2, pair_branch_shift)
    _, pair_dscore = score_grads(
        pair_scores, pair_max, pair_sum, pair_grad, pair_all_value, pair_delta
    )
    pair_dq = product(pair_dscore, pair_all_key, "hij,hjd->hid") * factor
    near_rows = (
        select(group_query, 2, pair_branch_shift),
        select(group_grad, 2, pair_branch_shift),
    )
    near_moments = (
        select(group_max, 2, pair_branch_shift),
        select(group_sum, 2, pair_branch_shift),
        select(group_delta, 2, pair_branch_shift),
    )
    all_query, all_grad = joined(
        near_rows, partner((near_rows[0], near_rows[1]), "seq", local_levels), local_levels
    )
    all_max, all_sum, all_delta = joined(
        near_moments,
        partner((near_moments[0], near_moments[1], near_moments[2]), "seq", local_levels),
        local_levels,
    )
    pair_back = masked(all_query, pair_key, 0, pair_rank * half_rows, factor)
    pair_back_prob, pair_back_dscore = score_grads(
        pair_back, all_max, all_sum, all_grad, pair_value, all_delta
    )
    pair_dk = product(pair_back_dscore, all_query, "hij,hid->hjd") * factor
    pair_dv = product(pair_back_prob, all_grad, "hij,hid->hjd")
    query_grad = query_grad + spread(pair_dq, 2, pair_branch_shift, 0.0)
    key_grad = key_grad + spread(pair_dk, 2, pair_branch_shift, 0.0)
    value_grad = value_grad + spread(pair_dv, 2, pair_branch_shift, 0.0)
    far_grad = select(head_grads, dilation, far_branch_shift)
    far_max = select(row_max, dilation, far_branch_shift)
    far_sum = select(row_sum, dilation, far_branch_shift)
    far_delta = select(row_delta, dilation, far_branch_shift)
    far_prob, far_dscore = score_grads(
        far_scores, far_max, far_sum, far_grad, every_value, far_delta
    )
    far_dq = product(far_dscore, every_key, "hij,hjd->hid") * factor
    gathered_dk = product(far_dscore, far_query, "hij,hid->hjd") * factor
    gathered_dv = product(far_prob, far_grad, "hij,hid->hjd")
    far_dk, far_dv = (
        lax.psum_scatter(gathered_dk, "seq", scatter_dimension=1, tiled=True),
        lax.psum_scatter(gathered_dv, "seq", scatter_dimension=1, tiled=True),
    )
    query_grad = query_grad + spread(far_dq, dilation, far_branch_shift, 0.0)
    key_grad = key_grad + spread(far_dk, dilation, far_branch_shift, 0.0)
    value_grad = value_grad + spread(far_dv, dilation, far_branch_shift, 0.0)
    return (
        layer_out,
        by_token(query_grad).astype(jnp.bfloat16),
        by_token(key_grad).astype(jnp.bfloat16),
        by_token(value_grad).astype(jnp.bfloat16),
    )


def lanes(index):
    return pl.ds(pl.multiple_of(index * HEAD_DIM, HEAD_DIM), HEAD_DIM)


def rows(index, length):
    return pl.ds(pl.multiple_of(index * length, length), length)


def matmul(left, right, dims):
    return lax.dot_general(left, right, (dims, ((), ())), preferred_element_type=jnp.float32)


NN = ((1,), (0,))
NT = ((1,), (1,))
TN = ((0,), (0,))


def call(body, out_shape, in_specs, scratch=(), flops=0, out_space=pltpu.VMEM, limit=40):
    out_spec = pl.BlockSpec(memory_space=out_space)
    return pl.pallas_call(
        body,
        out_shape=out_shape,
        in_specs=in_specs,
        out_specs=jax.tree.map(lambda _: out_spec, out_shape),
        scratch_shapes=list(scratch),
        cost_estimate=pl.CostEstimate(flops=flops, bytes_accessed=0, transcendentals=0),
        compiler_params=pltpu.CompilerParams(vmem_limit_bytes=limit * 2**20 if limit else None),
    )


def fast_local(plan, queries, key_rows, value_rows, out_weight, grad_out, pair_offsets, far_offsets):
    tokens, heads, group, selected, dilation, _ = plan
    factor = HEAD_DIM ** (-0.5)
    width = heads * HEAD_DIM
    model = out_weight.shape[1]
    span = group * tokens
    far_span = span // dilation
    bf16, f32 = jnp.bfloat16, jnp.float32
    vmem = pl.BlockSpec(memory_space=pltpu.VMEM)
    smem = pl.BlockSpec(memory_space=pltpu.SMEM)
    dests = range(group)

    def shape(extent, dtype=bf16):
        return jax.ShapeDtypeStruct(extent, dtype)

    def seq_rank():
        return lax.rem(lax.axis_index("seq"), group)

    def late_half():
        return lax.axis_index("seq") // group

    def my_head():
        return lax.axis_index("head") * heads + seq_rank()

    def swap(value, axis, mask):
        pairs = [(s, s ^ mask) for s in range(lax.axis_size(axis))]
        return lax.ppermute(value, axis, pairs)

    def swapped(blocks):
        return [blocks[0]] + [swap(blocks[m], "seq", m) for m in dests if m]

    mates = swap(grad_out, "head", 1)
    facing = swap(grad_out, "head", 2)
    relayed = swap(facing, "head", 1)

    def opening(out):
        out[...] = jnp.zeros_like(out)

    opened = call(opening, shape((8, HEAD_DIM), f32), [], flops=2 * 10**10)()

    def pack(opened, q, k, v, *outs):
        rank = seq_rank()
        for slot, ref in enumerate((q, k, v)):
            for m in dests:
                outs[m][:, slot * HEAD_DIM : (slot + 1) * HEAD_DIM] = ref[:, lanes(rank ^ m)]

    packed = call(
        pack, [shape((tokens, 3 * HEAD_DIM))] * group, [vmem] * 4, flops=10**9
    )(opened, queries, key_rows, value_rows)
    blocks = swapped(packed)

    def locate(po, fo, pair_start, far_start):
        pair_start[...] = jnp.full(pair_start.shape, po[my_head()], jnp.int32)
        far_start[...] = jnp.full(far_start.shape, fo[my_head()], jnp.int32)

    pair_start, far_start = call(
        locate, [shape((8, HEAD_DIM), jnp.int32)] * 2, [smem, smem], flops=10**6
    )(pair_offsets, far_offsets)

    def grad_term(w, part, mask):
        cols = lax.axis_index("head") ^ mask
        return matmul(part[...], w[:, pl.ds(pl.multiple_of(cols * width, width), width)], NT)

    def project_grad(w, *refs):
        parts, acc = refs[:-1], refs[-1]
        acc[...] = sum(grad_term(w, part, mask) for mask, part in enumerate(parts))

    def project_last(w, acc, facing, relayed, *refs):
        outs, (total,) = refs[:group], refs[group:]
        total[...] = acc[...] + grad_term(w, facing, 2) + grad_term(w, relayed, 3)
        rank = seq_rank()
        for m in dests:
            outs[m][...] = total[:, lanes(rank ^ m)].astype(bf16)

    partial_grad = call(
        project_grad, shape((tokens, width), f32), [vmem] * 3, flops=10**8
    )(out_weight, grad_out, mates)
    grad_blocks = swapped(
        call(
            project_last,
            [shape((tokens, HEAD_DIM))] * group,
            [vmem] * 4,
            [pltpu.VMEM((tokens, width), f32)],
            flops=10**8,
        )(out_weight, partial_grad, facing, relayed),
    )

    def branch_scores(query, key, mask):
        return jnp.where(mask, matmul(query, key, NT) * factor, masked_score)

    def causal(extent, shift=0):
        row_ids = lax.broadcasted_iota(jnp.int32, extent, 0)
        col_ids = lax.broadcasted_iota(jnp.int32, extent, 1)
        return row_ids + shift >= col_ids

    def far_mask():
        extent = (far_span, 2 * far_span)
        col_ids = lax.broadcasted_iota(jnp.int32, extent, 1)
        open_cols = jnp.where(late_half() > 0, 0, far_span)
        return causal(extent, far_span) & (col_ids >= open_cols)

    def stats(scores, value):
        top = jnp.max(scores, axis=-1, keepdims=True)
        weights = jnp.exp(scores - top)
        total = jnp.sum(weights, axis=-1, keepdims=True)
        return top, total, matmul(weights.astype(bf16), value, NN)

    def spread_lanes(column):
        return jnp.broadcast_to(column, (column.shape[0], HEAD_DIM))

    def pick(ref, at):
        return ref[at, :].astype(bf16)

    def pair_rows(po):
        return pl.ds(po[...][0, 0], selected, stride=2)

    def far_rows(fo):
        return pl.ds(fo[...][0, 0], far_span, stride=dilation)

    def with_early(early_kv, slot, ref, at):
        cols = slice(slot * HEAD_DIM, (slot + 1) * HEAD_DIM)
        return jnp.concatenate([early_kv[:, cols], pick(ref, at)], axis=0)

    wide = shape((span, HEAD_DIM), f32)
    far_pair = shape((far_span, 2 * HEAD_DIM))

    def assemble(fo, *refs):
        parts, (q, k, v, far_kv) = refs[:group], refs[group:]
        rank = seq_rank()
        for m in dests:
            at = rows(rank ^ m, tokens)
            for slot, ref in enumerate((q, k, v)):
                part = parts[m][:, slot * HEAD_DIM : (slot + 1) * HEAD_DIM]
                ref[at, :] = part.astype(f32)
        far_at = far_rows(fo)
        far_kv[:, :HEAD_DIM] = pick(k, far_at)
        far_kv[:, HEAD_DIM:] = pick(v, far_at)

    q, k, v, far_kv = call(
        assemble, [wide] * 3 + [far_pair], [vmem] + [vmem] * group, flops=10**7
    )(far_start, *blocks)
    early_kv = swap(far_kv, "seq", group)

    def forward_near(po, q, k, v, top_all, sum_all, acc):
        mask = causal((selected, selected))
        for first in range(0, span, selected):
            at = pl.ds(first, selected)
            top, total, numerator = stats(
                branch_scores(pick(q, at), pick(k, at), mask), pick(v, at)
            )
            top_all[at, :] = spread_lanes(top)
            sum_all[at, :] = spread_lanes(total)
            acc[at, :] = numerator
        merge(
            pair_rows(po),
            stats(
                branch_scores(pick(q, pair_rows(po)), pick(k, pair_rows(po)), mask),
                pick(v, pair_rows(po)),
            ),
            (top_all, sum_all, acc),
        )

    def merge(at, branch, totals):
        top, total, numerator = branch
        top_all, sum_all, acc = totals
        old_top = top_all[at, :]
        new_top = jnp.maximum(old_top, spread_lanes(top))
        old_scale, scale = jnp.exp(old_top - new_top), jnp.exp(top - new_top)
        top_all[at, :] = new_top
        sum_all[at, :] = sum_all[at, :] * old_scale + total * scale
        acc[at, :] = acc[at, :] * old_scale + numerator * scale

    near = call(forward_near, [wide] * 3, [vmem] + [vmem] * 3, flops=2 * 10**8)(
        pair_start, q, k, v
    )

    def forward_far(fo, q, k, v, early_kv, near_top, near_sum, near_acc, *refs):
        outs, (out_wide, lse, top_all, sum_all) = refs[:group], refs[group:]
        far_at = far_rows(fo)
        top_all[...] = near_top[...]
        sum_all[...] = near_sum[...]
        out_wide[...] = near_acc[...]
        key, value = with_early(early_kv, 0, k, far_at), with_early(early_kv, 1, v, far_at)
        branch = stats(branch_scores(pick(q, far_at), key, far_mask()), value)
        merge(far_at, branch, (top_all, sum_all, out_wide))
        out_wide[...] = out_wide[...] / sum_all[...]
        lse[...] = top_all[...] + jnp.log(sum_all[...])
        rank = seq_rank()
        for m in dests:
            outs[m][...] = out_wide[rows(rank ^ m, tokens), :].astype(bf16)

    scratch = pltpu.VMEM((span, HEAD_DIM), f32)
    *out_blocks, out_wide, lse = call(
        forward_far,
        [shape((tokens, HEAD_DIM))] * group + [wide, wide],
        [vmem] + [vmem] * 7,
        [scratch] * 2,
        flops=10**8,
    )(far_start, q, k, v, early_kv, *near)
    attended = swapped(out_blocks)

    def grads_of(query, key, value, grad, row_lse, row_delta, mask):
        scores = branch_scores(query, key, mask)
        probability = jnp.exp(scores - row_lse[:, :1])
        prob_grad = matmul(grad, value, NT)
        score_grad = (probability * (prob_grad - row_delta[:, :1])).astype(bf16)
        return (
            matmul(score_grad, key, NN) * factor,
            matmul(score_grad, query, TN) * factor,
            matmul(probability.astype(bf16), grad, TN),
        )

    def backward_far(fo, q, k, v, early_kv, out_wide, lse, *refs):
        parts, (grad, delta, far_dq, far_dk, far_dv, far_kv) = refs[:group], refs[group:]
        rank = seq_rank()
        for m in dests:
            grad[rows(rank ^ m, tokens), :] = parts[m][...].astype(f32)
        delta[...] = spread_lanes(jnp.sum(grad[...] * out_wide[...], axis=-1, keepdims=True))
        at = far_rows(fo)
        far_dq[...], dk, dv = grads_of(
            pick(q, at),
            with_early(early_kv, 0, k, at),
            with_early(early_kv, 1, v, at),
            pick(grad, at),
            lse[at, :],
            delta[at, :],
            far_mask(),
        )
        far_kv[:, :HEAD_DIM] = dk[:far_span].astype(bf16)
        far_kv[:, HEAD_DIM:] = dv[:far_span].astype(bf16)
        far_dk[...] = dk[far_span:]
        far_dv[...] = dv[far_span:]

    far_wide = shape((far_span, HEAD_DIM), f32)
    grad, delta, far_dq, far_dk, far_dv, late_kv = call(
        backward_far,
        [wide, wide] + [far_wide] * 3 + [far_pair],
        [vmem] + [vmem] * (6 + group),
        flops=2 * 10**8,
    )(far_start, q, k, v, early_kv, out_wide, lse, *grad_blocks)
    late = swap(late_kv, "seq", group)

    def near_grads(q, k, v, grad, lse, delta, at):
        mask = causal((selected, selected))
        return grads_of(
            pick(q, at), pick(k, at), pick(v, at), pick(grad, at), lse[at, :], delta[at, :], mask
        )

    def backward_pair(po, q, k, v, grad, lse, delta, *outs):
        for ref, term in zip(outs, near_grads(q, k, v, grad, lse, delta, pair_rows(po))):
            ref[...] = term

    pair_wide = shape((selected, HEAD_DIM), f32)
    pair_grads = call(backward_pair, [pair_wide] * 3, [vmem] * 7, flops=2 * 10**8)(
        pair_start, q, k, v, grad, lse, delta
    )

    def backward_local(po, fo, q, k, v, grad, lse, delta, *refs):
        pairs, fars, near = refs[:3], refs[3:6], refs[6:]
        for first in range(0, span, selected):
            at = pl.ds(first, selected)
            for ref, term in zip(near, near_grads(q, k, v, grad, lse, delta, at)):
                ref[at, :] = term
        for ref, pair, far in zip(near, pairs, fars):
            ref[pair_rows(po), :] += pair[...]
            ref[far_rows(fo), :] += far[...]

    dq, dk, dv = call(backward_local, [wide] * 3, [vmem] * 14, flops=4 * 10**8)(
        pair_start, far_start, q, k, v, grad, lse, delta, *pair_grads, far_dq, far_dk, far_dv
    )

    def finish(fo, dq, dk, dv, late, *refs):
        outs, sums = refs[:group], refs[group:]
        at = far_rows(fo)
        for slot, (ref, part) in enumerate(zip(sums, (dk, dv))):
            ref[...] = part[...]
            ref[at, :] += late[:, slot * HEAD_DIM : (slot + 1) * HEAD_DIM].astype(f32)
        rank = seq_rank()
        for m in dests:
            for slot, ref in enumerate((dq, *sums)):
                cols = slice(slot * HEAD_DIM, (slot + 1) * HEAD_DIM)
                outs[m][:, cols] = ref[rows(rank ^ m, tokens), :].astype(bf16)

    returned = swapped(
        call(
            finish,
            [shape((tokens, 3 * HEAD_DIM))] * group,
            [vmem] + [vmem] * 4,
            [scratch] * 2,
            flops=10**7,
        )(far_start, dq, dk, dv, late),
    )

    half = model // 2

    def columns(bit):
        return pl.ds(pl.multiple_of(bit * half, half), half)

    def my_half():
        return lax.rem(lax.axis_index("head"), 2)

    def project_theirs(w, *refs):
        parts, (both, send) = refs[:group], refs[group:]
        rank = seq_rank()
        for m in dests:
            both[:, lanes(rank ^ m)] = parts[m][...]
        send[...] = matmul(both[...], w[:, columns(1 - my_half())], NN).astype(bf16)

    half_out = shape((tokens, half))
    both, theirs = call(
        project_theirs,
        [shape((tokens, width)), half_out],
        [vmem] * (1 + group),
        flops=10**8,
    )(out_weight, *attended)
    mate = swap(theirs, "head", 1)

    def project_mine(w, both, out):
        out[...] = matmul(both[...], w[:, columns(my_half())], NN).astype(bf16)

    def add_mate(first, second, out):
        out[...] = (first[...].astype(f32) + second[...].astype(f32)).astype(bf16)

    def add_across(first, second, out):
        add_mate(first, second, out)

    mine = call(project_mine, half_out, [vmem] * 2, flops=10**8)(out_weight, both)
    pair_sum = call(add_mate, half_out, [vmem] * 2, flops=10**6)(mine, mate)
    across = swap(pair_sum, "head", 2)
    total = call(add_across, half_out, [vmem] * 2, flops=10**6)(pair_sum, across)
    other = swap(total, "head", 1)

    def copy_all(copies):
        for copy in copies:
            copy.start()
        for copy in copies:
            copy.wait()

    def close(mine, theirs, *refs):
        parts, out, outs, sems = refs[:group], refs[group], refs[group + 1 : group + 4], refs[-1]
        rank = seq_rank()
        copies = [
            (mine, out.at[:, columns(my_half())]),
            (theirs, out.at[:, columns(1 - my_half())]),
        ]
        copies += [
            (
                parts[m].at[:, slot * HEAD_DIM : (slot + 1) * HEAD_DIM],
                outs[slot].at[:, lanes(rank ^ m)],
            )
            for m in dests
            for slot in range(3)
        ]
        copy_all(
            [
                pltpu.make_async_copy(source, target, sems.at[number])
                for number, (source, target) in enumerate(copies)
            ]
        )

    return tuple(
        call(
            close,
            [shape((tokens, model))] + [shape((tokens, width))] * 3,
            [vmem] * (2 + group),
            [pltpu.SemaphoreType.DMA((2 + 3 * group,))],
            flops=10**7,
            out_space=pltpu.HBM,
        )(total, other, *returned)
    )


def local(queries, key_rows, value_rows, out_weight, grad_out, pair_offsets, far_head_offsets):
    tokens = queries.shape[0]
    heads = queries.shape[1] // HEAD_DIM
    seq_count = lax.axis_size("seq")
    total = tokens * seq_count
    selected = min(SPAN, total // 4)
    group = 2 * selected // tokens
    operands = (
        queries, key_rows, value_rows, out_weight, grad_out, pair_offsets, far_head_offsets
    )
    if group == heads and seq_count == 2 * group and lax.axis_size("head") == 4:
        plan = (tokens, heads, group, selected, total // selected, lax.axis_size("head"))
        return fast_local(plan, *operands)
    return exchange_local(*operands)


def solution(mesh):
    placed = (
        P("seq", "head"),
        P("seq", "head"),
        P("seq", "head"),
        P("head", None),
        P("seq", "head"),
        P(),
        P(),
    )
    return jax.shard_map(
        local,
        mesh=mesh,
        in_specs=placed,
        out_specs=(P("seq", None), P("seq", "head"), P("seq", "head"), P("seq", "head")),
        check_vma=False,
    )
```

```python
import jax
import jax.numpy as jnp
from jax import lax
from jax.experimental import pallas as pl
from jax.experimental.pallas import tpu as pltpu
from jax.sharding import PartitionSpec as P

HEAD_DIM = 128
SPAN = 512


masked_score = -1e30


def shortened(array):
    return jax.tree.map(lambda a: a.astype(jnp.bfloat16) if a.dtype == jnp.float32 else a, array)


def partner(value, axis, distance):
    mask = 2**distance
    pairs = [(source, source ^ mask) for source in range(lax.axis_size(axis))]
    return lax.ppermute(value, axis, pairs)


def select(tensor, token_stride, start_offset):
    head_count = tensor.shape[0]
    number = tensor.shape[1] // token_stride
    shaped = tensor.reshape((head_count, number, token_stride) + tensor.shape[2:])
    lane_ids = lax.broadcasted_iota(jnp.int32, shaped.shape, 2)
    chosen = start_offset.reshape((head_count, 1, 1) + (1,) * (tensor.ndim - 2))
    return jnp.sum(jnp.where(lane_ids == chosen, shaped, jnp.zeros((), tensor.dtype)), axis=2)


def spread(entries, token_stride, start_offset, filler):
    head_count = entries.shape[0]
    number = entries.shape[1]
    layout = (head_count, number, token_stride) + entries.shape[2:]
    lane_ids = lax.broadcasted_iota(jnp.int32, layout, 2)
    chosen = start_offset.reshape((head_count, 1, 1) + (1,) * (entries.ndim - 2))
    placed = jnp.where(lane_ids == chosen, jnp.expand_dims(entries, 2), filler)
    return placed.reshape((head_count, number * token_stride) + entries.shape[2:])


def product(left_side, right_side, pattern):
    return jnp.einsum(pattern, left_side, right_side, preferred_element_type=jnp.float32)


def masked(query_part, key_part, first_row, first_col, factor):
    scores = product(query_part, key_part, "hid,hjd->hij") * factor
    row_ids = first_row + lax.broadcasted_iota(jnp.int32, scores.shape, 1)
    col_ids = first_col + lax.broadcasted_iota(jnp.int32, scores.shape, 2)
    return jnp.where(row_ids >= col_ids, scores, masked_score)


def branch_stats(scores, value_part):
    branch_max = jnp.max(scores, axis=-1)
    weights = jnp.exp(scores - branch_max[..., None])
    numerator = product(weights.astype(jnp.bfloat16), value_part, "hij,hjd->hid")
    return (branch_max, jnp.sum(weights, axis=-1), numerator)


def score_grads(scores, row_max, row_sum, grad_part, value_part, row_delta):
    probability = jnp.exp(scores - row_max[..., None]) / row_sum[..., None]
    prob_grad = product(grad_part, value_part, "hid,hjd->hij")
    score_grad = (probability * (prob_grad - row_delta[..., None])).astype(jnp.bfloat16)
    return (probability.astype(jnp.bfloat16), score_grad)


def exchange_local(queries, key_rows, value_rows, out_weight, grad_out, pair_offsets, far_head_offsets):
    tokens = queries.shape[0]
    head_count = queries.shape[1] // HEAD_DIM
    factor = HEAD_DIM ** (-0.5)
    seq_count = lax.axis_size("seq")
    total = tokens * seq_count
    selected = min(SPAN, total // 4)
    local_group = selected // tokens
    local_levels = local_group.bit_length() - 1
    dilation = total // selected
    far_rows = tokens // dilation
    half_rows = tokens // 2
    position = lax.axis_index("seq")
    local_rank = position % local_group
    pair_rank = position % (2 * local_group)
    head_group = lax.axis_index("head")
    pair_branch_shift = lax.dynamic_slice_in_dim(pair_offsets, head_group * head_count, head_count)
    far_branch_shift = lax.dynamic_slice_in_dim(
        far_head_offsets, head_group * head_count, head_count
    )

    def by_head(tensor):
        return tensor.reshape(tokens, head_count, HEAD_DIM).transpose(1, 0, 2)

    def by_token(tensor):
        return tensor.transpose(1, 0, 2).reshape(tokens, head_count * HEAD_DIM)

    def stacked(mine, theirs, bit):
        high = position // 2**bit % 2 == 1
        lower = jnp.where(high, theirs, mine)
        upper = jnp.where(high, mine, theirs)
        return jnp.concatenate([lower, upper], axis=1)

    def joined(mine, theirs, bit):
        return tuple((stacked(first, second, bit) for first, second in zip(mine, theirs)))

    head_queries = by_head(queries)
    head_keys = by_head(key_rows)
    head_values = by_head(value_rows)
    parts = (head_keys, head_values)
    for bit in range(local_levels):
        parts = joined(
            parts,
            jax.tree.map(
                lambda part, own: part.astype(own.dtype),
                partner(shortened(parts), "seq", bit),
                parts,
            ),
            bit,
        )
    segment_key, segment_value = parts
    local_scores = masked(head_queries, segment_key, local_rank * tokens, 0, factor)
    local_stats = branch_stats(local_scores, segment_value)
    pair_query = select(head_queries, 2, pair_branch_shift)
    pair_key = select(head_keys, 2, pair_branch_shift)
    pair_value = select(head_values, 2, pair_branch_shift)
    nearby = (
        select(segment_key, 2, pair_branch_shift),
        select(segment_value, 2, pair_branch_shift),
    )
    pair_all_key, pair_all_value = joined(
        nearby, partner((nearby[0], nearby[1]), "seq", local_levels), local_levels
    )
    pair_scores = masked(pair_query, pair_all_key, pair_rank * half_rows, 0, factor)
    pair_stats = branch_stats(pair_scores, pair_all_value)
    far_query = select(head_queries, dilation, far_branch_shift)
    far_key = select(head_keys, dilation, far_branch_shift)
    far_value = select(head_values, dilation, far_branch_shift)
    every_key, every_value = (
        lax.all_gather(far_key, "seq", axis=1, tiled=True),
        lax.all_gather(far_value, "seq", axis=1, tiled=True),
    )
    far_scores = masked(far_query, every_key, position * far_rows, 0, factor)
    far_stats = branch_stats(far_scores, every_value)
    pair_spread = (
        spread(pair_stats[0], 2, pair_branch_shift, masked_score),
        spread(pair_stats[1], 2, pair_branch_shift, 0.0),
        spread(pair_stats[2], 2, pair_branch_shift, 0.0),
    )
    far_spread = (
        spread(far_stats[0], dilation, far_branch_shift, masked_score),
        spread(far_stats[1], dilation, far_branch_shift, 0.0),
        spread(far_stats[2], dilation, far_branch_shift, 0.0),
    )
    row_max = jnp.maximum(jnp.maximum(local_stats[0], pair_spread[0]), far_spread[0])
    row_sum = jnp.zeros_like(row_max)
    numerator = jnp.zeros_like(local_stats[2])
    for branch in (local_stats, pair_spread, far_spread):
        rescale = jnp.exp(branch[0] - row_max)
        row_sum = row_sum + branch[1] * rescale
        numerator = numerator + branch[2] * rescale[..., None]
    head_out = numerator / row_sum[..., None]
    attended = by_token(head_out).astype(jnp.bfloat16)
    partial_out = jnp.dot(attended, out_weight, preferred_element_type=jnp.float32)
    layer_out = lax.psum(partial_out.astype(jnp.bfloat16), "head")
    grad_attended = lax.dot_general(
        lax.all_gather(grad_out, "head", axis=1, tiled=True),
        out_weight,
        (((1,), (1,)), ((), ())),
        preferred_element_type=jnp.float32,
    )
    head_grads = by_head(grad_attended.astype(jnp.bfloat16))
    row_delta = jnp.sum(head_grads.astype(jnp.float32) * head_out, axis=-1)
    _, local_dscore = score_grads(
        local_scores, row_max, row_sum, head_grads, segment_value, row_delta
    )
    query_grad = product(local_dscore, segment_key, "hij,hjd->hid") * factor
    parts = (head_queries, head_grads)
    for bit in range(local_levels):
        parts = joined(
            parts,
            jax.tree.map(
                lambda part, own: part.astype(own.dtype),
                partner(shortened(parts), "seq", bit),
                parts,
            ),
            bit,
        )
    group_query, group_grad = parts
    parts = (row_max, row_sum, row_delta)
    for bit in range(local_levels):
        parts = joined(parts, partner(parts, "seq", bit), bit)
    group_max, group_sum, group_delta = parts
    back_scores = masked(group_query, head_keys, 0, local_rank * tokens, factor)
    back_prob, back_dscore = score_grads(
        back_scores, group_max, group_sum, group_grad, head_values, group_delta
    )
    key_grad = product(back_dscore, group_query, "hij,hid->hjd") * factor
    value_grad = product(back_prob, group_grad, "hij,hid->hjd")
    pair_grad = select(head_grads, 2, pair_branch_shift)
    pair_max = select(row_max, 2, pair_branch_shift)
    pair_sum = select(row_sum, 2, pair_branch_shift)
    pair_delta = select(row_delta, 2, pair_branch_shift)
    _, pair_dscore = score_grads(
        pair_scores, pair_max, pair_sum, pair_grad, pair_all_value, pair_delta
    )
    pair_dq = product(pair_dscore, pair_all_key, "hij,hjd->hid") * factor
    near_rows = (
        select(group_query, 2, pair_branch_shift),
        select(group_grad, 2, pair_branch_shift),
    )
    near_moments = (
        select(group_max, 2, pair_branch_shift),
        select(group_sum, 2, pair_branch_shift),
        select(group_delta, 2, pair_branch_shift),
    )
    all_query, all_grad = joined(
        near_rows, partner((near_rows[0], near_rows[1]), "seq", local_levels), local_levels
    )
    all_max, all_sum, all_delta = joined(
        near_moments,
        partner((near_moments[0], near_moments[1], near_moments[2]), "seq", local_levels),
        local_levels,
    )
    pair_back = masked(all_query, pair_key, 0, pair_rank * half_rows, factor)
    pair_back_prob, pair_back_dscore = score_grads(
        pair_back, all_max, all_sum, all_grad, pair_value, all_delta
    )
    pair_dk = product(pair_back_dscore, all_query, "hij,hid->hjd") * factor
    pair_dv = product(pair_back_prob, all_grad, "hij,hid->hjd")
    query_grad = query_grad + spread(pair_dq, 2, pair_branch_shift, 0.0)
    key_grad = key_grad + spread(pair_dk, 2, pair_branch_shift, 0.0)
    value_grad = value_grad + spread(pair_dv, 2, pair_branch_shift, 0.0)
    far_grad = select(head_grads, dilation, far_branch_shift)
    far_max = select(row_max, dilation, far_branch_shift)
    far_sum = select(row_sum, dilation, far_branch_shift)
    far_delta = select(row_delta, dilation, far_branch_shift)
    far_prob, far_dscore = score_grads(
        far_scores, far_max, far_sum, far_grad, every_value, far_delta
    )
    far_dq = product(far_dscore, every_key, "hij,hjd->hid") * factor
    gathered_dk = product(far_dscore, far_query, "hij,hid->hjd") * factor
    gathered_dv = product(far_prob, far_grad, "hij,hid->hjd")
    far_dk, far_dv = (
        lax.psum_scatter(gathered_dk, "seq", scatter_dimension=1, tiled=True),
        lax.psum_scatter(gathered_dv, "seq", scatter_dimension=1, tiled=True),
    )
    query_grad = query_grad + spread(far_dq, dilation, far_branch_shift, 0.0)
    key_grad = key_grad + spread(far_dk, dilation, far_branch_shift, 0.0)
    value_grad = value_grad + spread(far_dv, dilation, far_branch_shift, 0.0)
    return (
        layer_out,
        by_token(query_grad).astype(jnp.bfloat16),
        by_token(key_grad).astype(jnp.bfloat16),
        by_token(value_grad).astype(jnp.bfloat16),
    )


def lanes(index):
    return pl.ds(pl.multiple_of(index * HEAD_DIM, HEAD_DIM), HEAD_DIM)


def rows(index, length):
    return pl.ds(pl.multiple_of(index * length, length), length)


def matmul(left, right, dims):
    return lax.dot_general(left, right, (dims, ((), ())), preferred_element_type=jnp.float32)


NN = ((1,), (0,))
NT = ((1,), (1,))
TN = ((0,), (0,))


def call(body, out_shape, in_specs, scratch=(), flops=0, out_space=pltpu.VMEM, limit=40, aliases=None):
    out_spec = pl.BlockSpec(memory_space=out_space)
    return pl.pallas_call(
        body,
        out_shape=out_shape,
        in_specs=in_specs,
        out_specs=jax.tree.map(lambda _: out_spec, out_shape),
        scratch_shapes=list(scratch),
        input_output_aliases=aliases or {},
        cost_estimate=pl.CostEstimate(flops=flops, bytes_accessed=0, transcendentals=0),
        compiler_params=pltpu.CompilerParams(vmem_limit_bytes=limit * 2**20 if limit else None),
    )


def fast_local(plan, queries, key_rows, value_rows, out_weight, grad_out, pair_offsets, far_offsets):
    tokens, heads, group, selected, dilation, _ = plan
    factor = HEAD_DIM ** (-0.5)
    width = heads * HEAD_DIM
    model = out_weight.shape[1]
    span = group * tokens
    far_span = span // dilation
    bf16, f32 = jnp.bfloat16, jnp.float32
    vmem = pl.BlockSpec(memory_space=pltpu.VMEM)
    smem = pl.BlockSpec(memory_space=pltpu.SMEM)
    dests = range(group)

    def shape(extent, dtype=bf16):
        return jax.ShapeDtypeStruct(extent, dtype)

    def seq_rank():
        return lax.rem(lax.axis_index("seq"), group)

    def late_half():
        return lax.axis_index("seq") // group

    def my_head():
        return lax.axis_index("head") * heads + seq_rank()

    def swap(value, axis, mask):
        pairs = [(s, s ^ mask) for s in range(lax.axis_size(axis))]
        return lax.ppermute(value, axis, pairs)

    def swapped(blocks):
        return [blocks[0]] + [swap(blocks[m], "seq", m) for m in dests if m]

    mates = swap(grad_out, "head", 1)
    facing = swap(grad_out, "head", 2)
    relayed = swap(facing, "head", 1)

    def opening(out):
        out[...] = jnp.zeros_like(out)

    opened = call(opening, shape((8, HEAD_DIM), f32), [], flops=2 * 10**10)()

    def pack(opened, q, k, v, *outs):
        rank = seq_rank()
        for slot, ref in enumerate((q, k, v)):
            for m in dests:
                outs[m][:, slot * HEAD_DIM : (slot + 1) * HEAD_DIM] = ref[:, lanes(rank ^ m)]

    packed = call(
        pack, [shape((tokens, 3 * HEAD_DIM))] * group, [vmem] * 4, flops=10**9
    )(opened, queries, key_rows, value_rows)
    blocks = swapped(packed)

    def locate(po, fo, pair_start, far_start):
        pair_start[...] = jnp.full(pair_start.shape, po[my_head()], jnp.int32)
        far_start[...] = jnp.full(far_start.shape, fo[my_head()], jnp.int32)

    pair_start, far_start = call(
        locate, [shape((8, HEAD_DIM), jnp.int32)] * 2, [smem, smem], flops=10**6
    )(pair_offsets, far_offsets)

    def grad_term(w, part, mask):
        cols = lax.axis_index("head") ^ mask
        return matmul(part[...], w[:, pl.ds(pl.multiple_of(cols * width, width), width)], NT)

    def project_grad(w, *refs):
        parts, acc = refs[:-1], refs[-1]
        acc[...] = sum(grad_term(w, part, mask) for mask, part in enumerate(parts))

    def project_last(w, acc, facing, relayed, *refs):
        outs, (total,) = refs[:group], refs[group:]
        total[...] = acc[...] + grad_term(w, facing, 2) + grad_term(w, relayed, 3)
        rank = seq_rank()
        for m in dests:
            outs[m][...] = total[:, lanes(rank ^ m)].astype(bf16)

    partial_grad = call(
        project_grad, shape((tokens, width), f32), [vmem] * 3, flops=10**8
    )(out_weight, grad_out, mates)
    grad_blocks = swapped(
        call(
            project_last,
            [shape((tokens, HEAD_DIM))] * group,
            [vmem] * 4,
            [pltpu.VMEM((tokens, width), f32)],
            flops=10**8,
        )(out_weight, partial_grad, facing, relayed),
    )

    def branch_scores(query, key, mask):
        return jnp.where(mask, matmul(query, key, NT) * factor, masked_score)

    def causal(extent, shift=0):
        row_ids = lax.broadcasted_iota(jnp.int32, extent, 0)
        col_ids = lax.broadcasted_iota(jnp.int32, extent, 1)
        return row_ids + shift >= col_ids

    def far_mask():
        extent = (far_span, 2 * far_span)
        col_ids = lax.broadcasted_iota(jnp.int32, extent, 1)
        open_cols = jnp.where(late_half() > 0, 0, far_span)
        return causal(extent, far_span) & (col_ids >= open_cols)

    def stats(scores, value):
        top = jnp.max(scores, axis=-1, keepdims=True)
        weights = jnp.exp(scores - top)
        total = jnp.sum(weights, axis=-1, keepdims=True)
        return top, total, matmul(weights.astype(bf16), value, NN)

    def spread_lanes(column):
        return jnp.broadcast_to(column, (column.shape[0], HEAD_DIM))

    def pick(ref, at):
        return ref[at, :].astype(bf16)

    def pair_rows(po):
        return pl.ds(po[...][0, 0], selected, stride=2)

    def far_rows(fo):
        return pl.ds(fo[...][0, 0], far_span, stride=dilation)

    def with_early(early_kv, slot, ref, at):
        cols = slice(slot * HEAD_DIM, (slot + 1) * HEAD_DIM)
        return jnp.concatenate([early_kv[:, cols], pick(ref, at)], axis=0)

    wide = shape((span, HEAD_DIM), f32)
    far_pair = shape((far_span, 2 * HEAD_DIM))

    def assemble(fo, *refs):
        parts, (q, k, v, far_kv) = refs[:group], refs[group:]
        rank = seq_rank()
        for m in dests:
            at = rows(rank ^ m, tokens)
            for slot, ref in enumerate((q, k, v)):
                part = parts[m][:, slot * HEAD_DIM : (slot + 1) * HEAD_DIM]
                ref[at, :] = part.astype(f32)
        far_at = far_rows(fo)
        far_kv[:, :HEAD_DIM] = pick(k, far_at)
        far_kv[:, HEAD_DIM:] = pick(v, far_at)

    q, k, v, far_kv = call(
        assemble, [wide] * 3 + [far_pair], [vmem] + [vmem] * group, flops=10**7
    )(far_start, *blocks)
    early_kv = swap(far_kv, "seq", group)

    def near_rows(po, q, k, v, out, lse):
        mask = causal((selected, selected))
        for first in range(0, span, selected):
            at = pl.ds(first, selected)
            top, total, numerator = stats(
                branch_scores(pick(q, at), pick(k, at), mask), pick(v, at)
            )
            out[at, :] = numerator / total
            lse[at, :] = spread_lanes(top + jnp.log(total))
        at = pair_rows(po)
        merge(
            at, stats(branch_scores(pick(q, at), pick(k, at), mask), pick(v, at)), out, lse
        )

    def merge(at, branch, out, lse):
        top, total, numerator = branch
        old, new = lse[at, :], spread_lanes(top + jnp.log(total))
        peak = jnp.maximum(old, new)
        merged = peak + jnp.log(jnp.exp(old - peak) + jnp.exp(new - peak))
        out[at, :] = out[at, :] * jnp.exp(old - merged) + numerator / total * jnp.exp(new - merged)
        lse[at, :] = merged

    def forward_near(po, fo, q, k, v, out, lse):
        @pl.when(late_half() == 0)
        def _():
            near_rows(po, q, k, v, out, lse)
            at = far_rows(fo)
            scores = branch_scores(pick(q, at), pick(k, at), causal((far_span, far_span)))
            merge(at, stats(scores, pick(v, at)), out, lse)

    def forward_next(po, q, k, v, _, __, out, lse):
        @pl.when(late_half() > 0)
        def _():
            near_rows(po, q, k, v, out, lse)

    near = call(forward_near, [wide] * 2, [vmem] * 5, flops=2 * 10**8)(
        pair_start, far_start, q, k, v
    )
    near = call(
        forward_next, [wide] * 2, [vmem] * 6, flops=2 * 10**8, aliases={4: 0, 5: 1}
    )(pair_start, q, k, v, *near)

    def forward_far(fo, q, k, v, early_kv, _, __, *refs):
        outs, (out_wide, lse) = refs[:group], refs[group:]

        @pl.when(late_half() > 0)
        def _():
            at = far_rows(fo)
            key, value = with_early(early_kv, 0, k, at), with_early(early_kv, 1, v, at)
            scores = branch_scores(pick(q, at), key, causal((far_span, 2 * far_span), far_span))
            merge(at, stats(scores, value), out_wide, lse)

        rank = seq_rank()
        for m in dests:
            outs[m][...] = out_wide[rows(rank ^ m, tokens), :].astype(bf16)

    scratch = pltpu.VMEM((span, HEAD_DIM), f32)
    *out_blocks, out_wide, lse = call(
        forward_far,
        [shape((tokens, HEAD_DIM))] * group + [wide, wide],
        [vmem] * 7,
        flops=10**8,
        aliases={5: group, 6: group + 1},
    )(far_start, q, k, v, early_kv, *near)
    attended = swapped(out_blocks)

    def grads_of(query, key, value, grad, row_lse, row_delta, mask):
        scores = branch_scores(query, key, mask)
        probability = jnp.exp(scores - row_lse[:, :1])
        prob_grad = matmul(grad, value, NT)
        score_grad = (probability * (prob_grad - row_delta[:, :1])).astype(bf16)
        return (
            matmul(score_grad, key, NN) * factor,
            matmul(score_grad, query, TN) * factor,
            matmul(probability.astype(bf16), grad, TN),
        )

    def backward_far(fo, q, k, v, early_kv, out_wide, lse, *refs):
        parts, (grad, delta, far_dq, far_dk, far_dv, far_kv) = refs[:group], refs[group:]
        rank = seq_rank()
        for m in dests:
            grad[rows(rank ^ m, tokens), :] = parts[m][...].astype(f32)
        delta[...] = spread_lanes(jnp.sum(grad[...] * out_wide[...], axis=-1, keepdims=True))
        at = far_rows(fo)
        far_dq[...], dk, dv = grads_of(
            pick(q, at),
            with_early(early_kv, 0, k, at),
            with_early(early_kv, 1, v, at),
            pick(grad, at),
            lse[at, :],
            delta[at, :],
            far_mask(),
        )
        far_kv[:, :HEAD_DIM] = dk[:far_span].astype(bf16)
        far_kv[:, HEAD_DIM:] = dv[:far_span].astype(bf16)
        far_dk[...] = dk[far_span:]
        far_dv[...] = dv[far_span:]

    far_wide = shape((far_span, HEAD_DIM), f32)
    grad, delta, far_dq, far_dk, far_dv, late_kv = call(
        backward_far,
        [wide, wide] + [far_wide] * 3 + [far_pair],
        [vmem] + [vmem] * (6 + group),
        flops=2 * 10**8,
    )(far_start, q, k, v, early_kv, out_wide, lse, *grad_blocks)
    late = swap(late_kv, "seq", group)

    def near_grads(q, k, v, grad, lse, delta, at):
        mask = causal((selected, selected))
        return grads_of(
            pick(q, at), pick(k, at), pick(v, at), pick(grad, at), lse[at, :], delta[at, :], mask
        )

    def backward_pair(po, q, k, v, grad, lse, delta, *outs):
        for ref, term in zip(outs, near_grads(q, k, v, grad, lse, delta, pair_rows(po))):
            ref[...] = term

    pair_wide = shape((selected, HEAD_DIM), f32)
    pair_grads = call(backward_pair, [pair_wide] * 3, [vmem] * 7, flops=2 * 10**8)(
        pair_start, q, k, v, grad, lse, delta
    )

    def backward_local(po, fo, q, k, v, grad, lse, delta, *refs):
        pairs, fars, near = refs[:3], refs[3:6], refs[6:]
        for first in range(0, span, selected):
            at = pl.ds(first, selected)
            for ref, term in zip(near, near_grads(q, k, v, grad, lse, delta, at)):
                ref[at, :] = term
        for ref, pair, far in zip(near, pairs, fars):
            ref[pair_rows(po), :] += pair[...]
            ref[far_rows(fo), :] += far[...]

    dq, dk, dv = call(backward_local, [wide] * 3, [vmem] * 14, flops=4 * 10**8)(
        pair_start, far_start, q, k, v, grad, lse, delta, *pair_grads, far_dq, far_dk, far_dv
    )

    def finish(fo, dq, dk, dv, late, *refs):
        outs, sums = refs[:group], refs[group:]
        at = far_rows(fo)
        for slot, (ref, part) in enumerate(zip(sums, (dk, dv))):
            ref[...] = part[...]
            ref[at, :] += late[:, slot * HEAD_DIM : (slot + 1) * HEAD_DIM].astype(f32)
        rank = seq_rank()
        for m in dests:
            for slot, ref in enumerate((dq, *sums)):
                cols = slice(slot * HEAD_DIM, (slot + 1) * HEAD_DIM)
                outs[m][:, cols] = ref[rows(rank ^ m, tokens), :].astype(bf16)

    returned = swapped(
        call(
            finish,
            [shape((tokens, 3 * HEAD_DIM))] * group,
            [vmem] + [vmem] * 4,
            [scratch] * 2,
            flops=10**7,
        )(far_start, dq, dk, dv, late),
    )

    half = model // 2

    def columns(bit):
        return pl.ds(pl.multiple_of(bit * half, half), half)

    def my_half():
        return lax.rem(lax.axis_index("head"), 2)

    def project_theirs(w, *refs):
        parts, (both, send) = refs[:group], refs[group:]
        rank = seq_rank()
        for m in dests:
            both[:, lanes(rank ^ m)] = parts[m][...]
        send[...] = matmul(both[...], w[:, columns(1 - my_half())], NN).astype(bf16)

    half_out = shape((tokens, half))
    both, theirs = call(
        project_theirs,
        [shape((tokens, width)), half_out],
        [vmem] * (1 + group),
        flops=10**8,
    )(out_weight, *attended)
    mate = swap(theirs, "head", 1)

    def project_mine(w, both, out):
        out[...] = matmul(both[...], w[:, columns(my_half())], NN).astype(bf16)

    def add_mate(first, second, out):
        out[...] = (first[...].astype(f32) + second[...].astype(f32)).astype(bf16)

    def add_across(first, second, out):
        add_mate(first, second, out)

    mine = call(project_mine, half_out, [vmem] * 2, flops=10**8)(out_weight, both)
    pair_sum = call(add_mate, half_out, [vmem] * 2, flops=10**6)(mine, mate)
    across = swap(pair_sum, "head", 2)
    total = call(add_across, half_out, [vmem] * 2, flops=10**6)(pair_sum, across)
    other = swap(total, "head", 1)

    def copy_all(copies):
        for copy in copies:
            copy.start()
        for copy in copies:
            copy.wait()

    def close(mine, *refs):
        parts, out, outs, sems = refs[:group], refs[group], refs[group + 1 : group + 4], refs[-1]
        rank = seq_rank()
        copies = [(mine, out.at[:, columns(my_half())])] + [
            (
                parts[m].at[:, slot * HEAD_DIM : (slot + 1) * HEAD_DIM],
                outs[slot].at[:, lanes(rank ^ m)],
            )
            for m in dests
            for slot in range(3)
        ]
        copy_all(
            [
                pltpu.make_async_copy(source, target, sems.at[number])
                for number, (source, target) in enumerate(copies)
            ]
        )

    half_layer, *gradients = call(
        close,
        [shape((tokens, model))] + [shape((tokens, width))] * 3,
        [vmem] * (1 + group),
        [pltpu.SemaphoreType.DMA((1 + 3 * group,))],
        flops=10**7,
        out_space=pltpu.HBM,
    )(total, *returned)

    def join(theirs, _, out, sem):
        copy_all([pltpu.make_async_copy(theirs, out.at[:, columns(1 - my_half())], sem)])

    layer_out = call(
        join,
        shape((tokens, model)),
        [vmem, pl.BlockSpec(memory_space=pltpu.HBM)],
        [pltpu.SemaphoreType.DMA],
        flops=10**6,
        out_space=pltpu.HBM,
        aliases={1: 0},
    )(other, half_layer)
    return (layer_out, *gradients)


def local(queries, key_rows, value_rows, out_weight, grad_out, pair_offsets, far_head_offsets):
    tokens = queries.shape[0]
    heads = queries.shape[1] // HEAD_DIM
    seq_count = lax.axis_size("seq")
    total = tokens * seq_count
    selected = min(SPAN, total // 4)
    group = 2 * selected // tokens
    operands = (
        queries, key_rows, value_rows, out_weight, grad_out, pair_offsets, far_head_offsets
    )
    if group == heads and seq_count == 2 * group and lax.axis_size("head") == 4:
        plan = (tokens, heads, group, selected, total // selected, lax.axis_size("head"))
        return fast_local(plan, *operands)
    return exchange_local(*operands)


def solution(mesh):
    placed = (
        P("seq", "head"),
        P("seq", "head"),
        P("seq", "head"),
        P("head", None),
        P("seq", "head"),
        P(),
        P(),
    )
    return jax.shard_map(
        local,
        mesh=mesh,
        in_specs=placed,
        out_specs=(P("seq", None), P("seq", "head"), P("seq", "head"), P("seq", "head")),
        check_vma=False,
    )
```

```python
import jax
import jax.numpy as jnp
from jax import lax
from jax.experimental import pallas as pl
from jax.experimental.pallas import tpu as pltpu
from jax.sharding import PartitionSpec as P

SEQ = "seq"
HEAD = "head"
TO_KEYS = "hij,hid->hjd"
TO_ROWS = "hij,hjd->hid"
TO_SCORES = "hid,hjd->hij"
HEAD_DIM = 128
SPAN = 512


masked_score = -1e30


def shortened(array):
    return jax.tree.map(lambda a: a.astype(jnp.bfloat16) if a.dtype == jnp.float32 else a, array)


def partner(value, axis, distance):
    mask = 2**distance
    pairs = [(source, source ^ mask) for source in range(lax.axis_size(axis))]
    return lax.ppermute(value, axis, pairs)


def select(tensor, token_stride, start_offset):
    head_count = tensor.shape[0]
    number = tensor.shape[1] // token_stride
    shaped = tensor.reshape((head_count, number, token_stride) + tensor.shape[2:])
    lane_ids = lax.broadcasted_iota(jnp.int32, shaped.shape, 2)
    chosen = start_offset.reshape((head_count, 1, 1) + (1,) * (tensor.ndim - 2))
    return jnp.sum(jnp.where(lane_ids == chosen, shaped, jnp.zeros((), tensor.dtype)), axis=2)


def spread(entries, token_stride, start_offset, filler):
    head_count = entries.shape[0]
    number = entries.shape[1]
    layout = (head_count, number, token_stride) + entries.shape[2:]
    lane_ids = lax.broadcasted_iota(jnp.int32, layout, 2)
    chosen = start_offset.reshape((head_count, 1, 1) + (1,) * (entries.ndim - 2))
    placed = jnp.where(lane_ids == chosen, jnp.expand_dims(entries, 2), filler)
    return placed.reshape((head_count, number * token_stride) + entries.shape[2:])


def product(left_side, right_side, pattern):
    return jnp.einsum(pattern, left_side, right_side, preferred_element_type=jnp.float32)


def masked(query_part, key_part, first_row, first_col, factor):
    scores = product(query_part, key_part, TO_SCORES) * factor
    row_ids = first_row + lax.broadcasted_iota(jnp.int32, scores.shape, 1)
    col_ids = first_col + lax.broadcasted_iota(jnp.int32, scores.shape, 2)
    return jnp.where(row_ids >= col_ids, scores, masked_score)


def branch_stats(scores, value_part):
    branch_max = jnp.max(scores, axis=-1)
    weights = jnp.exp(scores - branch_max[..., None])
    numerator = product(weights.astype(jnp.bfloat16), value_part, TO_ROWS)
    return (branch_max, jnp.sum(weights, axis=-1), numerator)


def score_grads(scores, row_max, row_sum, grad_part, value_part, row_delta):
    probability = jnp.exp(scores - row_max[..., None]) / row_sum[..., None]
    prob_grad = product(grad_part, value_part, TO_SCORES)
    score_grad = (probability * (prob_grad - row_delta[..., None])).astype(jnp.bfloat16)
    return (probability.astype(jnp.bfloat16), score_grad)


def exchange_local(queries, key_rows, value_rows, out_weight, grad_out, pair_offsets, far_head_offsets):
    tokens = queries.shape[0]
    head_count = queries.shape[1] // HEAD_DIM
    factor = HEAD_DIM ** (-0.5)
    seq_count = lax.axis_size(SEQ)
    total = tokens * seq_count
    selected = min(SPAN, total // 4)
    local_group = selected // tokens
    local_levels = local_group.bit_length() - 1
    dilation = total // selected
    far_rows = tokens // dilation
    half_rows = tokens // 2
    position = lax.axis_index(SEQ)
    local_rank = position % local_group
    pair_rank = position % (2 * local_group)
    head_group = lax.axis_index(HEAD)
    pair_branch_shift = lax.dynamic_slice_in_dim(pair_offsets, head_group * head_count, head_count)
    far_branch_shift = lax.dynamic_slice_in_dim(
        far_head_offsets, head_group * head_count, head_count
    )

    def by_head(tensor):
        return tensor.reshape(tokens, head_count, HEAD_DIM).transpose(1, 0, 2)

    def by_token(tensor):
        return tensor.transpose(1, 0, 2).reshape(tokens, head_count * HEAD_DIM)

    def stacked(mine, theirs, bit):
        high = position // 2**bit % 2 == 1
        lower = jnp.where(high, theirs, mine)
        upper = jnp.where(high, mine, theirs)
        return jnp.concatenate([lower, upper], axis=1)

    def joined(mine, theirs, bit):
        return tuple((stacked(first, second, bit) for first, second in zip(mine, theirs)))

    head_queries = by_head(queries)
    head_keys = by_head(key_rows)
    head_values = by_head(value_rows)
    parts = (head_keys, head_values)
    for bit in range(local_levels):
        parts = joined(
            parts,
            jax.tree.map(
                lambda part, own: part.astype(own.dtype),
                partner(shortened(parts), SEQ, bit),
                parts,
            ),
            bit,
        )
    segment_key, segment_value = parts
    local_scores = masked(head_queries, segment_key, local_rank * tokens, 0, factor)
    local_stats = branch_stats(local_scores, segment_value)
    pair_query = select(head_queries, 2, pair_branch_shift)
    pair_key = select(head_keys, 2, pair_branch_shift)
    pair_value = select(head_values, 2, pair_branch_shift)
    nearby = (
        select(segment_key, 2, pair_branch_shift),
        select(segment_value, 2, pair_branch_shift),
    )
    pair_all_key, pair_all_value = joined(
        nearby, partner((nearby[0], nearby[1]), SEQ, local_levels), local_levels
    )
    pair_scores = masked(pair_query, pair_all_key, pair_rank * half_rows, 0, factor)
    pair_stats = branch_stats(pair_scores, pair_all_value)
    far_query = select(head_queries, dilation, far_branch_shift)
    far_key = select(head_keys, dilation, far_branch_shift)
    far_value = select(head_values, dilation, far_branch_shift)
    every_key, every_value = (
        lax.all_gather(far_key, SEQ, axis=1, tiled=True),
        lax.all_gather(far_value, SEQ, axis=1, tiled=True),
    )
    far_scores = masked(far_query, every_key, position * far_rows, 0, factor)
    far_stats = branch_stats(far_scores, every_value)
    pair_spread = (
        spread(pair_stats[0], 2, pair_branch_shift, masked_score),
        spread(pair_stats[1], 2, pair_branch_shift, 0.0),
        spread(pair_stats[2], 2, pair_branch_shift, 0.0),
    )
    far_spread = (
        spread(far_stats[0], dilation, far_branch_shift, masked_score),
        spread(far_stats[1], dilation, far_branch_shift, 0.0),
        spread(far_stats[2], dilation, far_branch_shift, 0.0),
    )
    row_max = jnp.maximum(jnp.maximum(local_stats[0], pair_spread[0]), far_spread[0])
    row_sum = jnp.zeros_like(row_max)
    numerator = jnp.zeros_like(local_stats[2])
    for branch in (local_stats, pair_spread, far_spread):
        rescale = jnp.exp(branch[0] - row_max)
        row_sum = row_sum + branch[1] * rescale
        numerator = numerator + branch[2] * rescale[..., None]
    head_out = numerator / row_sum[..., None]
    attended = by_token(head_out).astype(jnp.bfloat16)
    partial_out = jnp.dot(attended, out_weight, preferred_element_type=jnp.float32)
    layer_out = lax.psum(partial_out.astype(jnp.bfloat16), HEAD)
    grad_attended = lax.dot_general(
        lax.all_gather(grad_out, HEAD, axis=1, tiled=True),
        out_weight,
        (((1,), (1,)), ((), ())),
        preferred_element_type=jnp.float32,
    )
    head_grads = by_head(grad_attended.astype(jnp.bfloat16))
    row_delta = jnp.sum(head_grads.astype(jnp.float32) * head_out, axis=-1)
    _, local_dscore = score_grads(
        local_scores, row_max, row_sum, head_grads, segment_value, row_delta
    )
    query_grad = product(local_dscore, segment_key, TO_ROWS) * factor
    parts = (head_queries, head_grads)
    for bit in range(local_levels):
        parts = joined(
            parts,
            jax.tree.map(
                lambda part, own: part.astype(own.dtype),
                partner(shortened(parts), SEQ, bit),
                parts,
            ),
            bit,
        )
    group_query, group_grad = parts
    parts = (row_max, row_sum, row_delta)
    for bit in range(local_levels):
        parts = joined(parts, partner(parts, SEQ, bit), bit)
    group_max, group_sum, group_delta = parts
    back_scores = masked(group_query, head_keys, 0, local_rank * tokens, factor)
    back_prob, back_dscore = score_grads(
        back_scores, group_max, group_sum, group_grad, head_values, group_delta
    )
    key_grad = product(back_dscore, group_query, TO_KEYS) * factor
    value_grad = product(back_prob, group_grad, TO_KEYS)
    pair_grad = select(head_grads, 2, pair_branch_shift)
    pair_max = select(row_max, 2, pair_branch_shift)
    pair_sum = select(row_sum, 2, pair_branch_shift)
    pair_delta = select(row_delta, 2, pair_branch_shift)
    _, pair_dscore = score_grads(
        pair_scores, pair_max, pair_sum, pair_grad, pair_all_value, pair_delta
    )
    pair_dq = product(pair_dscore, pair_all_key, TO_ROWS) * factor
    near_rows = (
        select(group_query, 2, pair_branch_shift),
        select(group_grad, 2, pair_branch_shift),
    )
    near_moments = (
        select(group_max, 2, pair_branch_shift),
        select(group_sum, 2, pair_branch_shift),
        select(group_delta, 2, pair_branch_shift),
    )
    all_query, all_grad = joined(
        near_rows, partner((near_rows[0], near_rows[1]), SEQ, local_levels), local_levels
    )
    all_max, all_sum, all_delta = joined(
        near_moments,
        partner((near_moments[0], near_moments[1], near_moments[2]), SEQ, local_levels),
        local_levels,
    )
    pair_back = masked(all_query, pair_key, 0, pair_rank * half_rows, factor)
    pair_back_prob, pair_back_dscore = score_grads(
        pair_back, all_max, all_sum, all_grad, pair_value, all_delta
    )
    pair_dk = product(pair_back_dscore, all_query, TO_KEYS) * factor
    pair_dv = product(pair_back_prob, all_grad, TO_KEYS)
    query_grad = query_grad + spread(pair_dq, 2, pair_branch_shift, 0.0)
    key_grad = key_grad + spread(pair_dk, 2, pair_branch_shift, 0.0)
    value_grad = value_grad + spread(pair_dv, 2, pair_branch_shift, 0.0)
    far_grad = select(head_grads, dilation, far_branch_shift)
    far_max = select(row_max, dilation, far_branch_shift)
    far_sum = select(row_sum, dilation, far_branch_shift)
    far_delta = select(row_delta, dilation, far_branch_shift)
    far_prob, far_dscore = score_grads(
        far_scores, far_max, far_sum, far_grad, every_value, far_delta
    )
    far_dq = product(far_dscore, every_key, TO_ROWS) * factor
    gathered_dk = product(far_dscore, far_query, TO_KEYS) * factor
    gathered_dv = product(far_prob, far_grad, TO_KEYS)
    far_dk, far_dv = (
        lax.psum_scatter(gathered_dk, SEQ, scatter_dimension=1, tiled=True),
        lax.psum_scatter(gathered_dv, SEQ, scatter_dimension=1, tiled=True),
    )
    query_grad = query_grad + spread(far_dq, dilation, far_branch_shift, 0.0)
    key_grad = key_grad + spread(far_dk, dilation, far_branch_shift, 0.0)
    value_grad = value_grad + spread(far_dv, dilation, far_branch_shift, 0.0)
    return (
        layer_out,
        by_token(query_grad).astype(jnp.bfloat16),
        by_token(key_grad).astype(jnp.bfloat16),
        by_token(value_grad).astype(jnp.bfloat16),
    )


def lanes(index):
    return pl.ds(pl.multiple_of(index * HEAD_DIM, HEAD_DIM), HEAD_DIM)


def rows(index, length):
    return pl.ds(pl.multiple_of(index * length, length), length)


def matmul(left, right, dims):
    return lax.dot_general(left, right, (dims, ((), ())), preferred_element_type=jnp.float32)


NN = ((1,), (0,))
NT = ((1,), (1,))
TN = ((0,), (0,))


def call(body, out_shape, in_specs, scratch=(), flops=0, out_space=pltpu.VMEM, limit=40, aliases=None):
    out_spec = pl.BlockSpec(memory_space=out_space)
    return pl.pallas_call(
        body,
        out_shape=out_shape,
        in_specs=in_specs,
        out_specs=jax.tree.map(lambda _: out_spec, out_shape),
        scratch_shapes=list(scratch),
        input_output_aliases=aliases or {},
        cost_estimate=pl.CostEstimate(flops=flops, bytes_accessed=0, transcendentals=0),
        compiler_params=pltpu.CompilerParams(vmem_limit_bytes=limit * 2**20 if limit else None),
    )


def fast_local(plan, queries, key_rows, value_rows, out_weight, grad_out, pair_offsets, far_offsets):
    tokens, heads, group, selected, dilation, _ = plan
    factor = HEAD_DIM ** (-0.5)
    width = heads * HEAD_DIM
    model = out_weight.shape[1]
    span = group * tokens
    far_span = span // dilation
    bf16, f32 = jnp.bfloat16, jnp.float32
    vmem = pl.BlockSpec(memory_space=pltpu.VMEM)
    smem = pl.BlockSpec(memory_space=pltpu.SMEM)
    dests = range(group)

    def shape(extent, dtype=bf16):
        return jax.ShapeDtypeStruct(extent, dtype)

    def seq_rank():
        return lax.rem(lax.axis_index(SEQ), group)

    def late_half():
        return lax.axis_index(SEQ) // group

    def my_head():
        return lax.axis_index(HEAD) * heads + seq_rank()

    def swap(value, axis, mask):
        pairs = [(s, s ^ mask) for s in range(lax.axis_size(axis))]
        return lax.ppermute(value, axis, pairs)

    def swapped(blocks):
        return [blocks[0]] + [swap(blocks[m], SEQ, m) for m in dests if m]

    mates = swap(grad_out, HEAD, 1)
    facing = swap(grad_out, HEAD, 2)
    relayed = swap(facing, HEAD, 1)

    def opening(out):
        out[...] = jnp.zeros_like(out)

    opened = call(opening, shape((8, HEAD_DIM), f32), [], flops=2 * 10**10)()

    def pack(opened, q, k, v, *outs):
        rank = seq_rank()
        for slot, ref in enumerate((q, k, v)):
            for m in dests:
                outs[m][:, slot * HEAD_DIM : (slot + 1) * HEAD_DIM] = ref[:, lanes(rank ^ m)]

    packed = call(
        pack, [shape((tokens, 3 * HEAD_DIM))] * group, [vmem] * 4, flops=10**9
    )(opened, queries, key_rows, value_rows)
    blocks = swapped(packed)

    def locate(po, fo, pair_start, far_start):
        pair_start[...] = jnp.full(pair_start.shape, po[my_head()], jnp.int32)
        far_start[...] = jnp.full(far_start.shape, fo[my_head()], jnp.int32)

    pair_start, far_start = call(
        locate, [shape((8, HEAD_DIM), jnp.int32)] * 2, [smem, smem], flops=10**6
    )(pair_offsets, far_offsets)

    def grad_term(w, part, mask):
        cols = lax.axis_index(HEAD) ^ mask
        return matmul(part[...], w[:, pl.ds(pl.multiple_of(cols * width, width), width)], NT)

    def project_grad(w, *refs):
        parts, acc = refs[:-1], refs[-1]
        acc[...] = sum(grad_term(w, part, mask) for mask, part in enumerate(parts))

    def project_last(w, acc, facing, relayed, *refs):
        outs, (total,) = refs[:group], refs[group:]
        total[...] = acc[...] + grad_term(w, facing, 2) + grad_term(w, relayed, 3)
        rank = seq_rank()
        for m in dests:
            outs[m][...] = total[:, lanes(rank ^ m)].astype(bf16)

    partial_grad = call(
        project_grad, shape((tokens, width), f32), [vmem] * 3, flops=10**8
    )(out_weight, grad_out, mates)
    grad_blocks = swapped(
        call(
            project_last,
            [shape((tokens, HEAD_DIM))] * group,
            [vmem] * 4,
            [pltpu.VMEM((tokens, width), f32)],
            flops=10**8,
        )(out_weight, partial_grad, facing, relayed),
    )

    def branch_scores(query, key, mask):
        return jnp.where(mask, matmul(query, key, NT) * factor, masked_score)

    def causal(extent, shift=0):
        row_ids = lax.broadcasted_iota(jnp.int32, extent, 0)
        col_ids = lax.broadcasted_iota(jnp.int32, extent, 1)
        return row_ids + shift >= col_ids

    def far_mask():
        extent = (far_span, 2 * far_span)
        col_ids = lax.broadcasted_iota(jnp.int32, extent, 1)
        open_cols = jnp.where(late_half() > 0, 0, far_span)
        return causal(extent, far_span) & (col_ids >= open_cols)

    def stats(scores, value):
        top = jnp.max(scores, axis=-1, keepdims=True)
        weights = jnp.exp(scores - top)
        total = jnp.sum(weights, axis=-1, keepdims=True)
        return top, total, matmul(weights.astype(bf16), value, NN)

    def spread_lanes(column):
        return jnp.broadcast_to(column, (column.shape[0], HEAD_DIM))

    def pick(ref, at):
        return ref[at, :].astype(bf16)

    def pair_rows(po):
        return pl.ds(po[...][0, 0], selected, stride=2)

    def far_rows(fo):
        return pl.ds(fo[...][0, 0], far_span, stride=dilation)

    def with_early(early_kv, slot, ref, at):
        cols = slice(slot * HEAD_DIM, (slot + 1) * HEAD_DIM)
        return jnp.concatenate([early_kv[:, cols], pick(ref, at)], axis=0)

    wide = shape((span, HEAD_DIM), f32)
    far_pair = shape((far_span, 2 * HEAD_DIM))

    def assemble(fo, *refs):
        parts, (q, k, v, far_kv) = refs[:group], refs[group:]
        rank = seq_rank()
        for m in dests:
            at = rows(rank ^ m, tokens)
            for slot, ref in enumerate((q, k, v)):
                part = parts[m][:, slot * HEAD_DIM : (slot + 1) * HEAD_DIM]
                ref[at, :] = part.astype(f32)
        far_at = far_rows(fo)
        far_kv[:, :HEAD_DIM] = pick(k, far_at)
        far_kv[:, HEAD_DIM:] = pick(v, far_at)

    q, k, v, far_kv = call(
        assemble, [wide] * 3 + [far_pair], [vmem] + [vmem] * group, flops=10**7
    )(far_start, *blocks)
    early_kv = swap(far_kv, SEQ, group)

    def near_rows(po, q, k, v, out, lse):
        mask = causal((selected, selected))
        for first in range(0, span, selected):
            at = pl.ds(first, selected)
            top, total, numerator = stats(
                branch_scores(pick(q, at), pick(k, at), mask), pick(v, at)
            )
            out[at, :] = numerator / total
            lse[at, :] = spread_lanes(top + jnp.log(total))
        at = pair_rows(po)
        merge(
            at, stats(branch_scores(pick(q, at), pick(k, at), mask), pick(v, at)), out, lse
        )

    def merge(at, branch, out, lse):
        top, total, numerator = branch
        old, new = lse[at, :], spread_lanes(top + jnp.log(total))
        peak = jnp.maximum(old, new)
        merged = peak + jnp.log(jnp.exp(old - peak) + jnp.exp(new - peak))
        out[at, :] = out[at, :] * jnp.exp(old - merged) + numerator / total * jnp.exp(new - merged)
        lse[at, :] = merged

    def forward_near(po, fo, q, k, v, out, lse):
        @pl.when(late_half() == 0)
        def _():
            near_rows(po, q, k, v, out, lse)
            at = far_rows(fo)
            scores = branch_scores(pick(q, at), pick(k, at), causal((far_span, far_span)))
            merge(at, stats(scores, pick(v, at)), out, lse)

    def forward_next(po, q, k, v, _, __, out, lse):
        @pl.when(late_half() > 0)
        def _():
            near_rows(po, q, k, v, out, lse)

    near = call(forward_near, [wide] * 2, [vmem] * 5, flops=2 * 10**8)(
        pair_start, far_start, q, k, v
    )
    near = call(
        forward_next, [wide] * 2, [vmem] * 6, flops=2 * 10**8, aliases={4: 0, 5: 1}
    )(pair_start, q, k, v, *near)

    def forward_far(fo, q, k, v, early_kv, _, __, *refs):
        outs, (out_wide, lse) = refs[:group], refs[group:]

        @pl.when(late_half() > 0)
        def _():
            at = far_rows(fo)
            key, value = with_early(early_kv, 0, k, at), with_early(early_kv, 1, v, at)
            scores = branch_scores(pick(q, at), key, causal((far_span, 2 * far_span), far_span))
            merge(at, stats(scores, value), out_wide, lse)

        rank = seq_rank()
        for m in dests:
            outs[m][...] = out_wide[rows(rank ^ m, tokens), :].astype(bf16)

    scratch = pltpu.VMEM((span, HEAD_DIM), f32)
    *out_blocks, out_wide, lse = call(
        forward_far,
        [shape((tokens, HEAD_DIM))] * group + [wide, wide],
        [vmem] * 7,
        flops=10**8,
        aliases={5: group, 6: group + 1},
    )(far_start, q, k, v, early_kv, *near)
    attended = swapped(out_blocks)

    def grads_of(query, key, value, grad, row_lse, row_delta, mask):
        scores = branch_scores(query, key, mask)
        probability = jnp.exp(scores - row_lse[:, :1])
        prob_grad = matmul(grad, value, NT)
        score_grad = (probability * (prob_grad - row_delta[:, :1])).astype(bf16)
        return (
            matmul(score_grad, key, NN) * factor,
            matmul(score_grad, query, TN) * factor,
            matmul(probability.astype(bf16), grad, TN),
        )

    def backward_far(fo, q, k, v, early_kv, out_wide, lse, *refs):
        parts, (grad, delta, far_dq, far_dk, far_dv, far_kv) = refs[:group], refs[group:]
        rank = seq_rank()
        for m in dests:
            grad[rows(rank ^ m, tokens), :] = parts[m][...].astype(f32)
        delta[...] = spread_lanes(jnp.sum(grad[...] * out_wide[...], axis=-1, keepdims=True))
        at = far_rows(fo)
        far_dq[...], dk, dv = grads_of(
            pick(q, at),
            with_early(early_kv, 0, k, at),
            with_early(early_kv, 1, v, at),
            pick(grad, at),
            lse[at, :],
            delta[at, :],
            far_mask(),
        )
        far_kv[:, :HEAD_DIM] = dk[:far_span].astype(bf16)
        far_kv[:, HEAD_DIM:] = dv[:far_span].astype(bf16)
        far_dk[...] = dk[far_span:]
        far_dv[...] = dv[far_span:]

    far_wide = shape((far_span, HEAD_DIM), f32)
    grad, delta, far_dq, far_dk, far_dv, late_kv = call(
        backward_far,
        [wide, wide] + [far_wide] * 3 + [far_pair],
        [vmem] + [vmem] * (6 + group),
        flops=2 * 10**8,
    )(far_start, q, k, v, early_kv, out_wide, lse, *grad_blocks)
    late = swap(late_kv, SEQ, group)

    def near_grads(q, k, v, grad, lse, delta, at):
        mask = causal((selected, selected))
        return grads_of(
            pick(q, at), pick(k, at), pick(v, at), pick(grad, at), lse[at, :], delta[at, :], mask
        )

    def backward_pair(po, q, k, v, grad, lse, delta, *outs):
        for ref, term in zip(outs, near_grads(q, k, v, grad, lse, delta, pair_rows(po))):
            ref[...] = term

    pair_wide = shape((selected, HEAD_DIM), f32)
    pair_grads = call(backward_pair, [pair_wide] * 3, [vmem] * 7, flops=2 * 10**8)(
        pair_start, q, k, v, grad, lse, delta
    )

    def backward_local(po, fo, q, k, v, grad, lse, delta, *refs):
        pairs, fars, near = refs[:3], refs[3:6], refs[6:]
        for first in range(0, span, selected):
            at = pl.ds(first, selected)
            for ref, term in zip(near, near_grads(q, k, v, grad, lse, delta, at)):
                ref[at, :] = term
        for ref, pair, far in zip(near, pairs, fars):
            ref[pair_rows(po), :] += pair[...]
            ref[far_rows(fo), :] += far[...]

    dq, dk, dv = call(backward_local, [wide] * 3, [vmem] * 14, flops=4 * 10**8)(
        pair_start, far_start, q, k, v, grad, lse, delta, *pair_grads, far_dq, far_dk, far_dv
    )

    def finish(fo, dq, dk, dv, late, *refs):
        outs, sums = refs[:group], refs[group:]
        at = far_rows(fo)
        for slot, (ref, part) in enumerate(zip(sums, (dk, dv))):
            ref[...] = part[...]
            ref[at, :] += late[:, slot * HEAD_DIM : (slot + 1) * HEAD_DIM].astype(f32)
        rank = seq_rank()
        for m in dests:
            for slot, ref in enumerate((dq, *sums)):
                cols = slice(slot * HEAD_DIM, (slot + 1) * HEAD_DIM)
                outs[m][:, cols] = ref[rows(rank ^ m, tokens), :].astype(bf16)

    returned = swapped(
        call(
            finish,
            [shape((tokens, 3 * HEAD_DIM))] * group,
            [vmem] + [vmem] * 4,
            [scratch] * 2,
            flops=10**7,
        )(far_start, dq, dk, dv, late),
    )

    half = model // 2

    def columns(bit):
        return pl.ds(pl.multiple_of(bit * half, half), half)

    def my_half():
        return lax.rem(lax.axis_index(HEAD), 2)

    def project_theirs(w, *refs):
        parts, (both, send) = refs[:group], refs[group:]
        rank = seq_rank()
        for m in dests:
            both[:, lanes(rank ^ m)] = parts[m][...]
        send[...] = matmul(both[...], w[:, columns(1 - my_half())], NN).astype(bf16)

    half_out = shape((tokens, half))
    both, theirs = call(
        project_theirs,
        [shape((tokens, width)), half_out],
        [vmem] * (1 + group),
        flops=10**8,
    )(out_weight, *attended)
    mate = swap(theirs, HEAD, 1)

    def project_mine(w, both, out):
        out[...] = matmul(both[...], w[:, columns(my_half())], NN).astype(bf16)

    def add_mate(first, second, out):
        out[...] = (first[...].astype(f32) + second[...].astype(f32)).astype(bf16)

    def add_across(first, second, out):
        add_mate(first, second, out)

    mine = call(project_mine, half_out, [vmem] * 2, flops=10**8)(out_weight, both)
    pair_sum = call(add_mate, half_out, [vmem] * 2, flops=10**6)(mine, mate)
    across = swap(pair_sum, HEAD, 2)
    total = call(add_across, half_out, [vmem] * 2, flops=10**6)(pair_sum, across)
    other = swap(total, HEAD, 1)

    def copy_all(copies):
        for copy in copies:
            copy.start()
        for copy in copies:
            copy.wait()

    def close(mine, *refs):
        parts, out, outs, sems = refs[:group], refs[group], refs[group + 1 : group + 4], refs[-1]
        rank = seq_rank()
        copies = [(mine, out.at[:, columns(my_half())])] + [
            (
                parts[m].at[:, slot * HEAD_DIM : (slot + 1) * HEAD_DIM],
                outs[slot].at[:, lanes(rank ^ m)],
            )
            for m in dests
            for slot in range(3)
        ]
        copy_all(
            [
                pltpu.make_async_copy(source, target, sems.at[number])
                for number, (source, target) in enumerate(copies)
            ]
        )

    half_layer, *gradients = call(
        close,
        [shape((tokens, model))] + [shape((tokens, width))] * 3,
        [vmem] * (1 + group),
        [pltpu.SemaphoreType.DMA((1 + 3 * group,))],
        flops=10**7,
        out_space=pltpu.HBM,
    )(total, *returned)

    def join(theirs, _, out, sem):
        copy_all([pltpu.make_async_copy(theirs, out.at[:, columns(1 - my_half())], sem)])

    layer_out = call(
        join,
        shape((tokens, model)),
        [vmem, pl.BlockSpec(memory_space=pltpu.HBM)],
        [pltpu.SemaphoreType.DMA],
        flops=10**6,
        out_space=pltpu.HBM,
        aliases={1: 0},
    )(other, half_layer)
    return (layer_out, *gradients)


def local(queries, key_rows, value_rows, out_weight, grad_out, pair_offsets, far_head_offsets):
    tokens = queries.shape[0]
    heads = queries.shape[1] // HEAD_DIM
    seq_count = lax.axis_size(SEQ)
    total = tokens * seq_count
    selected = min(SPAN, total // 4)
    group = 2 * selected // tokens
    operands = (
        queries, key_rows, value_rows, out_weight, grad_out, pair_offsets, far_head_offsets
    )
    if group == heads and seq_count == 2 * group and lax.axis_size(HEAD) == 4:
        plan = (tokens, heads, group, selected, total // selected, lax.axis_size(HEAD))
        return fast_local(plan, *operands)
    return exchange_local(*operands)


def solution(mesh):
    placed = (
        P(SEQ, HEAD),
        P(SEQ, HEAD),
        P(SEQ, HEAD),
        P(HEAD, None),
        P(SEQ, HEAD),
        P(),
        P(),
    )
    return jax.shard_map(
        local,
        mesh=mesh,
        in_specs=placed,
        out_specs=(P(SEQ, None), P(SEQ, HEAD), P(SEQ, HEAD), P(SEQ, HEAD)),
        check_vma=False,
    )
```

```python
import jax
import jax.numpy as jnp
from jax import lax
from jax.experimental import pallas as pl
from jax.experimental.pallas import tpu as pltpu
from jax.sharding import PartitionSpec as P

SEQ = "seq"
HEAD = "head"
TO_KEYS = "hij,hid->hjd"
TO_ROWS = "hij,hjd->hid"
TO_SCORES = "hid,hjd->hij"
HEAD_DIM = 128
SPAN = 512


masked_score = -1e30


def shortened(array):
    return jax.tree.map(lambda a: a.astype(jnp.bfloat16) if a.dtype == jnp.float32 else a, array)


def partner(value, axis, distance):
    mask = 2**distance
    pairs = [(source, source ^ mask) for source in range(lax.axis_size(axis))]
    return lax.ppermute(value, axis, pairs)


def select(tensor, token_stride, start_offset):
    head_count = tensor.shape[0]
    number = tensor.shape[1] // token_stride
    shaped = tensor.reshape((head_count, number, token_stride) + tensor.shape[2:])
    lane_ids = lax.broadcasted_iota(jnp.int32, shaped.shape, 2)
    chosen = start_offset.reshape((head_count, 1, 1) + (1,) * (tensor.ndim - 2))
    return jnp.sum(jnp.where(lane_ids == chosen, shaped, jnp.zeros((), tensor.dtype)), axis=2)


def spread(entries, token_stride, start_offset, filler):
    head_count = entries.shape[0]
    number = entries.shape[1]
    layout = (head_count, number, token_stride) + entries.shape[2:]
    lane_ids = lax.broadcasted_iota(jnp.int32, layout, 2)
    chosen = start_offset.reshape((head_count, 1, 1) + (1,) * (entries.ndim - 2))
    placed = jnp.where(lane_ids == chosen, jnp.expand_dims(entries, 2), filler)
    return placed.reshape((head_count, number * token_stride) + entries.shape[2:])


def product(left_side, right_side, pattern):
    return jnp.einsum(pattern, left_side, right_side, preferred_element_type=jnp.float32)


def masked(query_part, key_part, first_row, first_col, factor):
    scores = product(query_part, key_part, TO_SCORES) * factor
    row_ids = first_row + lax.broadcasted_iota(jnp.int32, scores.shape, 1)
    col_ids = first_col + lax.broadcasted_iota(jnp.int32, scores.shape, 2)
    return jnp.where(row_ids >= col_ids, scores, masked_score)


def branch_stats(scores, value_part):
    branch_max = jnp.max(scores, axis=-1)
    weights = jnp.exp(scores - branch_max[..., None])
    numerator = product(weights.astype(jnp.bfloat16), value_part, TO_ROWS)
    return (branch_max, jnp.sum(weights, axis=-1), numerator)


def score_grads(scores, row_max, row_sum, grad_part, value_part, row_delta):
    probability = jnp.exp(scores - row_max[..., None]) / row_sum[..., None]
    prob_grad = product(grad_part, value_part, TO_SCORES)
    score_grad = (probability * (prob_grad - row_delta[..., None])).astype(jnp.bfloat16)
    return (probability.astype(jnp.bfloat16), score_grad)


def exchange_local(queries, key_rows, value_rows, out_weight, grad_out, pair_offsets, far_head_offsets):
    tokens = queries.shape[0]
    head_count = queries.shape[1] // HEAD_DIM
    factor = HEAD_DIM ** (-0.5)
    seq_count = lax.axis_size(SEQ)
    total = tokens * seq_count
    selected = min(SPAN, total // 4)
    local_group = selected // tokens
    local_levels = local_group.bit_length() - 1
    dilation = total // selected
    far_rows = tokens // dilation
    half_rows = tokens // 2
    position = lax.axis_index(SEQ)
    local_rank = position % local_group
    pair_rank = position % (2 * local_group)
    head_group = lax.axis_index(HEAD)
    pair_branch_shift = lax.dynamic_slice_in_dim(pair_offsets, head_group * head_count, head_count)
    far_branch_shift = lax.dynamic_slice_in_dim(
        far_head_offsets, head_group * head_count, head_count
    )

    def by_head(tensor):
        return tensor.reshape(tokens, head_count, HEAD_DIM).transpose(1, 0, 2)

    def by_token(tensor):
        return tensor.transpose(1, 0, 2).reshape(tokens, head_count * HEAD_DIM)

    def stacked(mine, theirs, bit):
        high = position // 2**bit % 2 == 1
        lower = jnp.where(high, theirs, mine)
        upper = jnp.where(high, mine, theirs)
        return jnp.concatenate([lower, upper], axis=1)

    def joined(mine, theirs, bit):
        return tuple((stacked(first, second, bit) for first, second in zip(mine, theirs)))

    head_queries = by_head(queries)
    head_keys = by_head(key_rows)
    head_values = by_head(value_rows)
    parts = (head_keys, head_values)
    for bit in range(local_levels):
        parts = joined(
            parts,
            jax.tree.map(
                lambda part, own: part.astype(own.dtype),
                partner(shortened(parts), SEQ, bit),
                parts,
            ),
            bit,
        )
    segment_key, segment_value = parts
    local_scores = masked(head_queries, segment_key, local_rank * tokens, 0, factor)
    local_stats = branch_stats(local_scores, segment_value)
    pair_query = select(head_queries, 2, pair_branch_shift)
    pair_key = select(head_keys, 2, pair_branch_shift)
    pair_value = select(head_values, 2, pair_branch_shift)
    nearby = (
        select(segment_key, 2, pair_branch_shift),
        select(segment_value, 2, pair_branch_shift),
    )
    pair_all_key, pair_all_value = joined(
        nearby, partner((nearby[0], nearby[1]), SEQ, local_levels), local_levels
    )
    pair_scores = masked(pair_query, pair_all_key, pair_rank * half_rows, 0, factor)
    pair_stats = branch_stats(pair_scores, pair_all_value)
    far_query = select(head_queries, dilation, far_branch_shift)
    far_key = select(head_keys, dilation, far_branch_shift)
    far_value = select(head_values, dilation, far_branch_shift)
    every_key, every_value = (
        lax.all_gather(far_key, SEQ, axis=1, tiled=True),
        lax.all_gather(far_value, SEQ, axis=1, tiled=True),
    )
    far_scores = masked(far_query, every_key, position * far_rows, 0, factor)
    far_stats = branch_stats(far_scores, every_value)
    pair_spread = (
        spread(pair_stats[0], 2, pair_branch_shift, masked_score),
        spread(pair_stats[1], 2, pair_branch_shift, 0.0),
        spread(pair_stats[2], 2, pair_branch_shift, 0.0),
    )
    far_spread = (
        spread(far_stats[0], dilation, far_branch_shift, masked_score),
        spread(far_stats[1], dilation, far_branch_shift, 0.0),
        spread(far_stats[2], dilation, far_branch_shift, 0.0),
    )
    row_max = jnp.maximum(jnp.maximum(local_stats[0], pair_spread[0]), far_spread[0])
    row_sum = jnp.zeros_like(row_max)
    numerator = jnp.zeros_like(local_stats[2])
    for branch in (local_stats, pair_spread, far_spread):
        rescale = jnp.exp(branch[0] - row_max)
        row_sum = row_sum + branch[1] * rescale
        numerator = numerator + branch[2] * rescale[..., None]
    head_out = numerator / row_sum[..., None]
    attended = by_token(head_out).astype(jnp.bfloat16)
    partial_out = jnp.dot(attended, out_weight, preferred_element_type=jnp.float32)
    layer_out = lax.psum(partial_out.astype(jnp.bfloat16), HEAD)
    grad_attended = lax.dot_general(
        lax.all_gather(grad_out, HEAD, axis=1, tiled=True),
        out_weight,
        (((1,), (1,)), ((), ())),
        preferred_element_type=jnp.float32,
    )
    head_grads = by_head(grad_attended.astype(jnp.bfloat16))
    row_delta = jnp.sum(head_grads.astype(jnp.float32) * head_out, axis=-1)
    _, local_dscore = score_grads(
        local_scores, row_max, row_sum, head_grads, segment_value, row_delta
    )
    query_grad = product(local_dscore, segment_key, TO_ROWS) * factor
    parts = (head_queries, head_grads)
    for bit in range(local_levels):
        parts = joined(
            parts,
            jax.tree.map(
                lambda part, own: part.astype(own.dtype),
                partner(shortened(parts), SEQ, bit),
                parts,
            ),
            bit,
        )
    group_query, group_grad = parts
    parts = (row_max, row_sum, row_delta)
    for bit in range(local_levels):
        parts = joined(parts, partner(parts, SEQ, bit), bit)
    group_max, group_sum, group_delta = parts
    back_scores = masked(group_query, head_keys, 0, local_rank * tokens, factor)
    back_prob, back_dscore = score_grads(
        back_scores, group_max, group_sum, group_grad, head_values, group_delta
    )
    key_grad = product(back_dscore, group_query, TO_KEYS) * factor
    value_grad = product(back_prob, group_grad, TO_KEYS)
    pair_grad = select(head_grads, 2, pair_branch_shift)
    pair_max = select(row_max, 2, pair_branch_shift)
    pair_sum = select(row_sum, 2, pair_branch_shift)
    pair_delta = select(row_delta, 2, pair_branch_shift)
    _, pair_dscore = score_grads(
        pair_scores, pair_max, pair_sum, pair_grad, pair_all_value, pair_delta
    )
    pair_dq = product(pair_dscore, pair_all_key, TO_ROWS) * factor
    near_rows = (
        select(group_query, 2, pair_branch_shift),
        select(group_grad, 2, pair_branch_shift),
    )
    near_moments = (
        select(group_max, 2, pair_branch_shift),
        select(group_sum, 2, pair_branch_shift),
        select(group_delta, 2, pair_branch_shift),
    )
    all_query, all_grad = joined(
        near_rows, partner((near_rows[0], near_rows[1]), SEQ, local_levels), local_levels
    )
    all_max, all_sum, all_delta = joined(
        near_moments,
        partner((near_moments[0], near_moments[1], near_moments[2]), SEQ, local_levels),
        local_levels,
    )
    pair_back = masked(all_query, pair_key, 0, pair_rank * half_rows, factor)
    pair_back_prob, pair_back_dscore = score_grads(
        pair_back, all_max, all_sum, all_grad, pair_value, all_delta
    )
    pair_dk = product(pair_back_dscore, all_query, TO_KEYS) * factor
    pair_dv = product(pair_back_prob, all_grad, TO_KEYS)
    query_grad = query_grad + spread(pair_dq, 2, pair_branch_shift, 0.0)
    key_grad = key_grad + spread(pair_dk, 2, pair_branch_shift, 0.0)
    value_grad = value_grad + spread(pair_dv, 2, pair_branch_shift, 0.0)
    far_grad = select(head_grads, dilation, far_branch_shift)
    far_max = select(row_max, dilation, far_branch_shift)
    far_sum = select(row_sum, dilation, far_branch_shift)
    far_delta = select(row_delta, dilation, far_branch_shift)
    far_prob, far_dscore = score_grads(
        far_scores, far_max, far_sum, far_grad, every_value, far_delta
    )
    far_dq = product(far_dscore, every_key, TO_ROWS) * factor
    gathered_dk = product(far_dscore, far_query, TO_KEYS) * factor
    gathered_dv = product(far_prob, far_grad, TO_KEYS)
    far_dk, far_dv = (
        lax.psum_scatter(gathered_dk, SEQ, scatter_dimension=1, tiled=True),
        lax.psum_scatter(gathered_dv, SEQ, scatter_dimension=1, tiled=True),
    )
    query_grad = query_grad + spread(far_dq, dilation, far_branch_shift, 0.0)
    key_grad = key_grad + spread(far_dk, dilation, far_branch_shift, 0.0)
    value_grad = value_grad + spread(far_dv, dilation, far_branch_shift, 0.0)
    return (
        layer_out,
        by_token(query_grad).astype(jnp.bfloat16),
        by_token(key_grad).astype(jnp.bfloat16),
        by_token(value_grad).astype(jnp.bfloat16),
    )


def lanes(index):
    return pl.ds(pl.multiple_of(index * HEAD_DIM, HEAD_DIM), HEAD_DIM)


def rows(index, length):
    return pl.ds(pl.multiple_of(index * length, length), length)


def matmul(left, right, dims):
    return lax.dot_general(left, right, (dims, ((), ())), preferred_element_type=jnp.float32)


NN = ((1,), (0,))
NT = ((1,), (1,))
TN = ((0,), (0,))


def call(body, out_shape, in_specs, scratch=(), flops=0, out_space=pltpu.VMEM, limit=40, aliases=None):
    out_spec = pl.BlockSpec(memory_space=out_space)
    return pl.pallas_call(
        body,
        out_shape=out_shape,
        in_specs=in_specs,
        out_specs=jax.tree.map(lambda _: out_spec, out_shape),
        scratch_shapes=list(scratch),
        input_output_aliases=aliases or {},
        cost_estimate=pl.CostEstimate(flops=flops, bytes_accessed=0, transcendentals=0),
        compiler_params=pltpu.CompilerParams(vmem_limit_bytes=limit * 2**20 if limit else None),
    )


def fast_local(plan, queries, key_rows, value_rows, out_weight, grad_out, pair_offsets, far_offsets):
    tokens, heads, group, selected, dilation, _ = plan
    factor = HEAD_DIM ** (-0.5)
    width = heads * HEAD_DIM
    model = out_weight.shape[1]
    span = group * tokens
    far_span = span // dilation
    bf16, f32 = jnp.bfloat16, jnp.float32
    vmem = pl.BlockSpec(memory_space=pltpu.VMEM)
    smem = pl.BlockSpec(memory_space=pltpu.SMEM)
    dests = range(group)

    def shape(extent, dtype=bf16):
        return jax.ShapeDtypeStruct(extent, dtype)

    def seq_rank():
        return lax.rem(lax.axis_index(SEQ), group)

    def late_half():
        return lax.axis_index(SEQ) // group

    def my_head():
        return lax.axis_index(HEAD) * heads + seq_rank()

    def swap(value, axis, mask):
        pairs = [(s, s ^ mask) for s in range(lax.axis_size(axis))]
        return lax.ppermute(value, axis, pairs)

    def swapped(blocks):
        return [blocks[0]] + [swap(blocks[m], SEQ, m) for m in dests if m]

    mates = swap(grad_out, HEAD, 1)
    facing = swap(grad_out, HEAD, 2)
    relayed = swap(facing, HEAD, 1)

    def opening(out):
        out[...] = jnp.zeros_like(out)

    opened = call(opening, shape((8, HEAD_DIM), f32), [], flops=2 * 10**10)()

    def pack(opened, q, k, v, *outs):
        rank = seq_rank()
        for slot, ref in enumerate((q, k, v)):
            for m in dests:
                outs[m][:, slot * HEAD_DIM : (slot + 1) * HEAD_DIM] = ref[:, lanes(rank ^ m)]

    packed = call(
        pack, [shape((tokens, 3 * HEAD_DIM))] * group, [vmem] * 4, flops=10**9
    )(opened, queries, key_rows, value_rows)
    blocks = swapped(packed)

    def locate(po, fo, pair_start, far_start):
        pair_start[...] = jnp.full(pair_start.shape, po[my_head()], jnp.int32)
        far_start[...] = jnp.full(far_start.shape, fo[my_head()], jnp.int32)

    pair_start, far_start = call(
        locate, [shape((8, HEAD_DIM), jnp.int32)] * 2, [smem, smem], flops=10**6
    )(pair_offsets, far_offsets)

    def grad_term(w, part, mask):
        cols = lax.axis_index(HEAD) ^ mask
        return matmul(part[...], w[:, pl.ds(pl.multiple_of(cols * width, width), width)], NT)

    def project_grad(w, *refs):
        parts, acc = refs[:-1], refs[-1]
        acc[...] = sum(grad_term(w, part, mask) for mask, part in enumerate(parts))

    def project_last(w, acc, facing, relayed, *refs):
        outs, (total,) = refs[:group], refs[group:]
        total[...] = acc[...] + grad_term(w, facing, 2) + grad_term(w, relayed, 3)
        rank = seq_rank()
        for m in dests:
            outs[m][...] = total[:, lanes(rank ^ m)].astype(bf16)

    partial_grad = call(
        project_grad, shape((tokens, width), f32), [vmem] * 3, flops=10**8
    )(out_weight, grad_out, mates)
    grad_blocks = swapped(
        call(
            project_last,
            [shape((tokens, HEAD_DIM))] * group,
            [vmem] * 4,
            [pltpu.VMEM((tokens, width), f32)],
            flops=10**8,
        )(out_weight, partial_grad, facing, relayed),
    )

    def branch_scores(query, key, mask):
        return jnp.where(mask, matmul(query, key, NT) * factor, masked_score)

    def causal(extent, shift=0):
        row_ids = lax.broadcasted_iota(jnp.int32, extent, 0)
        col_ids = lax.broadcasted_iota(jnp.int32, extent, 1)
        return row_ids + shift >= col_ids

    def far_mask():
        extent = (far_span, 2 * far_span)
        col_ids = lax.broadcasted_iota(jnp.int32, extent, 1)
        open_cols = jnp.where(late_half() > 0, 0, far_span)
        return causal(extent, far_span) & (col_ids >= open_cols)

    def stats(scores, value):
        top = jnp.max(scores, axis=-1, keepdims=True)
        weights = jnp.exp(scores - top)
        total = jnp.sum(weights, axis=-1, keepdims=True)
        return top, total, matmul(weights.astype(bf16), value, NN)

    def spread_lanes(column):
        return jnp.broadcast_to(column, (column.shape[0], HEAD_DIM))

    def pick(ref, at):
        return ref[at, :].astype(bf16)

    def pair_rows(po):
        return pl.ds(po[...][0, 0], selected, stride=2)

    def far_rows(fo):
        return pl.ds(fo[...][0, 0], far_span, stride=dilation)

    def with_early(early_kv, slot, ref, at):
        cols = slice(slot * HEAD_DIM, (slot + 1) * HEAD_DIM)
        return jnp.concatenate([early_kv[:, cols], pick(ref, at)], axis=0)

    wide = shape((span, HEAD_DIM), f32)
    far_pair = shape((far_span, 2 * HEAD_DIM))

    def assemble(fo, *refs):
        parts, (q, k, v, far_kv) = refs[:group], refs[group:]
        rank = seq_rank()
        for m in dests:
            at = rows(rank ^ m, tokens)
            for slot, ref in enumerate((q, k, v)):
                part = parts[m][:, slot * HEAD_DIM : (slot + 1) * HEAD_DIM]
                ref[at, :] = part.astype(f32)
        far_at = far_rows(fo)
        far_kv[:, :HEAD_DIM] = pick(k, far_at)
        far_kv[:, HEAD_DIM:] = pick(v, far_at)

    q, k, v, far_kv = call(
        assemble, [wide] * 3 + [far_pair], [vmem] + [vmem] * group, flops=10**7
    )(far_start, *blocks)
    early_kv = swap(far_kv, SEQ, group)

    def near_rows(po, q, k, v, out, lse):
        mask = causal((selected, selected))
        for first in range(0, span, selected):
            at = pl.ds(first, selected)
            top, total, numerator = stats(
                branch_scores(pick(q, at), pick(k, at), mask), pick(v, at)
            )
            out[at, :] = numerator / total
            lse[at, :] = spread_lanes(top + jnp.log(total))
        at = pair_rows(po)
        merge(
            at, stats(branch_scores(pick(q, at), pick(k, at), mask), pick(v, at)), out, lse
        )

    def merge(at, branch, out, lse):
        top, total, numerator = branch
        old, new = lse[at, :], spread_lanes(top + jnp.log(total))
        peak = jnp.maximum(old, new)
        merged = peak + jnp.log(jnp.exp(old - peak) + jnp.exp(new - peak))
        out[at, :] = out[at, :] * jnp.exp(old - merged) + numerator / total * jnp.exp(new - merged)
        lse[at, :] = merged

    def forward_near(po, fo, q, k, v, out, lse):
        @pl.when(late_half() == 0)
        def _():
            near_rows(po, q, k, v, out, lse)
            at = far_rows(fo)
            scores = branch_scores(pick(q, at), pick(k, at), causal((far_span, far_span)))
            merge(at, stats(scores, pick(v, at)), out, lse)

    def forward_next(po, q, k, v, _, __, out, lse):
        @pl.when(late_half() > 0)
        def _():
            near_rows(po, q, k, v, out, lse)

    near = call(forward_near, [wide] * 2, [vmem] * 5, flops=2 * 10**8)(
        pair_start, far_start, q, k, v
    )
    near = call(
        forward_next, [wide] * 2, [vmem] * 6, flops=2 * 10**8, aliases={4: 0, 5: 1}
    )(pair_start, q, k, v, *near)

    def forward_far(fo, q, k, v, early_kv, _, __, *refs):
        outs, (out_wide, lse) = refs[:group], refs[group:]

        @pl.when(late_half() > 0)
        def _():
            at = far_rows(fo)
            key, value = with_early(early_kv, 0, k, at), with_early(early_kv, 1, v, at)
            scores = branch_scores(pick(q, at), key, causal((far_span, 2 * far_span), far_span))
            merge(at, stats(scores, value), out_wide, lse)

        rank = seq_rank()
        for m in dests:
            outs[m][...] = out_wide[rows(rank ^ m, tokens), :].astype(bf16)

    scratch = pltpu.VMEM((span, HEAD_DIM), f32)
    *out_blocks, out_wide, lse = call(
        forward_far,
        [shape((tokens, HEAD_DIM))] * group + [wide, wide],
        [vmem] * 7,
        flops=10**8,
        aliases={5: group, 6: group + 1},
    )(far_start, q, k, v, early_kv, *near)
    attended = swapped(out_blocks)

    def grads_of(query, key, value, grad, row_lse, row_delta, mask):
        scores = branch_scores(query, key, mask)
        probability = jnp.exp(scores - row_lse[:, :1])
        prob_grad = matmul(grad, value, NT)
        score_grad = (probability * (prob_grad - row_delta[:, :1])).astype(bf16)
        return (
            matmul(score_grad, key, NN) * factor,
            matmul(score_grad, query, TN) * factor,
            matmul(probability.astype(bf16), grad, TN),
        )

    def backward_far(fo, q, k, v, early_kv, out_wide, lse, *refs):
        parts, (grad, delta, far_dq, far_dk, far_dv, far_kv) = refs[:group], refs[group:]
        rank = seq_rank()
        for m in dests:
            grad[rows(rank ^ m, tokens), :] = parts[m][...].astype(f32)
        delta[...] = spread_lanes(jnp.sum(grad[...] * out_wide[...], axis=-1, keepdims=True))
        at = far_rows(fo)
        far_dq[...], dk, dv = grads_of(
            pick(q, at),
            with_early(early_kv, 0, k, at),
            with_early(early_kv, 1, v, at),
            pick(grad, at),
            lse[at, :],
            delta[at, :],
            far_mask(),
        )
        far_kv[:, :HEAD_DIM] = dk[:far_span].astype(bf16)
        far_kv[:, HEAD_DIM:] = dv[:far_span].astype(bf16)
        far_dk[...] = dk[far_span:]
        far_dv[...] = dv[far_span:]

    far_wide = shape((far_span, HEAD_DIM), f32)
    grad, delta, far_dq, far_dk, far_dv, late_kv = call(
        backward_far,
        [wide, wide] + [far_wide] * 3 + [far_pair],
        [vmem] + [vmem] * (6 + group),
        flops=2 * 10**8,
    )(far_start, q, k, v, early_kv, out_wide, lse, *grad_blocks)
    late = swap(late_kv, SEQ, group)

    def near_grads(q, k, v, grad, lse, delta, at):
        mask = causal((selected, selected))
        return grads_of(
            pick(q, at), pick(k, at), pick(v, at), pick(grad, at), lse[at, :], delta[at, :], mask
        )

    def pair_terms(po, refs, outs):
        for ref, term in zip(outs, near_grads(*refs, pair_rows(po))):
            ref[...] = term

    def backward_pair(po, *refs):
        @pl.when(late_half() == 0)
        def _():
            pair_terms(po, refs[:6], refs[6:])

    def backward_next(po, *refs):
        @pl.when(late_half() > 0)
        def _():
            pair_terms(po, refs[:6], refs[9:])

    pair_wide = shape((selected, HEAD_DIM), f32)
    rows_in = (pair_start, q, k, v, grad, lse, delta)
    pair_grads = call(backward_pair, [pair_wide] * 3, [vmem] * 7, flops=2 * 10**8)(*rows_in)
    pair_grads = call(
        backward_next,
        [pair_wide] * 3,
        [vmem] * 10,
        flops=2 * 10**8,
        aliases={7: 0, 8: 1, 9: 2},
    )(*rows_in, *pair_grads)

    def backward_low(q, k, v, grad, lse, delta, *near):
        half_span = pl.ds(0, selected)
        for ref, term in zip(near, near_grads(q, k, v, grad, lse, delta, half_span)):
            ref[half_span, :] = term

    near = call(backward_low, [wide] * 3, [vmem] * 6, flops=2 * 10**8)(
        q, k, v, grad, lse, delta
    )

    def backward_high(po, fo, q, k, v, grad, lse, delta, *refs):
        pairs, fars, near = refs[:3], refs[3:6], refs[9:]
        for first in range(selected, span, selected):
            at = pl.ds(first, selected)
            for ref, term in zip(near, near_grads(q, k, v, grad, lse, delta, at)):
                ref[at, :] = term
        for ref, pair, far in zip(near, pairs, fars):
            ref[pair_rows(po), :] += pair[...]
            ref[far_rows(fo), :] += far[...]

    dq, dk, dv = call(
        backward_high,
        [wide] * 3,
        [vmem] * 17,
        flops=4 * 10**8,
        aliases={14: 0, 15: 1, 16: 2},
    )(
        pair_start,
        far_start,
        *(q, k, v, grad, lse, delta),
        *pair_grads,
        *(far_dq, far_dk, far_dv),
        *near,
    )

    def finish(fo, dq, dk, dv, late, *refs):
        outs, sums = refs[:group], refs[group:]
        at = far_rows(fo)
        for slot, (ref, part) in enumerate(zip(sums, (dk, dv))):
            ref[...] = part[...]
            ref[at, :] += late[:, slot * HEAD_DIM : (slot + 1) * HEAD_DIM].astype(f32)
        rank = seq_rank()
        for m in dests:
            for slot, ref in enumerate((dq, *sums)):
                cols = slice(slot * HEAD_DIM, (slot + 1) * HEAD_DIM)
                outs[m][:, cols] = ref[rows(rank ^ m, tokens), :].astype(bf16)

    returned = swapped(
        call(
            finish,
            [shape((tokens, 3 * HEAD_DIM))] * group,
            [vmem] + [vmem] * 4,
            [scratch] * 2,
            flops=10**7,
        )(far_start, dq, dk, dv, late),
    )

    half = model // 2

    def columns(bit):
        return pl.ds(pl.multiple_of(bit * half, half), half)

    def my_half():
        return lax.rem(lax.axis_index(HEAD), 2)

    def project_theirs(w, *refs):
        parts, (both, send) = refs[:group], refs[group:]
        rank = seq_rank()
        for m in dests:
            both[:, lanes(rank ^ m)] = parts[m][...]
        send[...] = matmul(both[...], w[:, columns(1 - my_half())], NN).astype(bf16)

    half_out = shape((tokens, half))
    both, theirs = call(
        project_theirs,
        [shape((tokens, width)), half_out],
        [vmem] * (1 + group),
        flops=10**8,
    )(out_weight, *attended)
    mate = swap(theirs, HEAD, 1)

    def project_mine(w, both, out):
        out[...] = matmul(both[...], w[:, columns(my_half())], NN).astype(bf16)

    def add_mate(first, second, out):
        out[...] = (first[...].astype(f32) + second[...].astype(f32)).astype(bf16)

    def add_across(first, second, out):
        add_mate(first, second, out)

    mine = call(project_mine, half_out, [vmem] * 2, flops=10**8)(out_weight, both)
    pair_sum = call(add_mate, half_out, [vmem] * 2, flops=10**6)(mine, mate)
    across = swap(pair_sum, HEAD, 2)
    total = call(add_across, half_out, [vmem] * 2, flops=10**6)(pair_sum, across)
    other = swap(total, HEAD, 1)

    def copy_all(copies):
        for copy in copies:
            copy.start()
        for copy in copies:
            copy.wait()

    def close(mine, *refs):
        parts, out, outs, sems = refs[:group], refs[group], refs[group + 1 : group + 4], refs[-1]
        rank = seq_rank()
        copies = [(mine, out.at[:, columns(my_half())])] + [
            (
                parts[m].at[:, slot * HEAD_DIM : (slot + 1) * HEAD_DIM],
                outs[slot].at[:, lanes(rank ^ m)],
            )
            for m in dests
            for slot in range(3)
        ]
        copy_all(
            [
                pltpu.make_async_copy(source, target, sems.at[number])
                for number, (source, target) in enumerate(copies)
            ]
        )

    half_layer, *gradients = call(
        close,
        [shape((tokens, model))] + [shape((tokens, width))] * 3,
        [vmem] * (1 + group),
        [pltpu.SemaphoreType.DMA((1 + 3 * group,))],
        flops=10**7,
        out_space=pltpu.HBM,
    )(total, *returned)

    def join(theirs, _, out, sem):
        copy_all([pltpu.make_async_copy(theirs, out.at[:, columns(1 - my_half())], sem)])

    layer_out = call(
        join,
        shape((tokens, model)),
        [vmem, pl.BlockSpec(memory_space=pltpu.HBM)],
        [pltpu.SemaphoreType.DMA],
        flops=10**6,
        out_space=pltpu.HBM,
        aliases={1: 0},
    )(other, half_layer)
    return (layer_out, *gradients)


def local(queries, key_rows, value_rows, out_weight, grad_out, pair_offsets, far_head_offsets):
    tokens = queries.shape[0]
    heads = queries.shape[1] // HEAD_DIM
    seq_count = lax.axis_size(SEQ)
    total = tokens * seq_count
    selected = min(SPAN, total // 4)
    group = 2 * selected // tokens
    operands = (
        queries, key_rows, value_rows, out_weight, grad_out, pair_offsets, far_head_offsets
    )
    if group == heads and seq_count == 2 * group and lax.axis_size(HEAD) == 4:
        plan = (tokens, heads, group, selected, total // selected, lax.axis_size(HEAD))
        return fast_local(plan, *operands)
    return exchange_local(*operands)


def solution(mesh):
    placed = (
        P(SEQ, HEAD),
        P(SEQ, HEAD),
        P(SEQ, HEAD),
        P(HEAD, None),
        P(SEQ, HEAD),
        P(),
        P(),
    )
    return jax.shard_map(
        local,
        mesh=mesh,
        in_specs=placed,
        out_specs=(P(SEQ, None), P(SEQ, HEAD), P(SEQ, HEAD), P(SEQ, HEAD)),
        check_vma=False,
    )
```
